32 devices in a mesh: req: 2 (over y), patch: 16 (over z, x, core).
Axes of the slice: x: 2, y: 2, z: 4, core: 2. Of those that a mesh axis runs over, the one named last changes fastest.
Arguments:
- tokens: bfloat16 [1536, 1152], P(('req', 'patch')), parts along dimension 0, may hold values from -6 to 6
- positions: int32 [2, 1536], P(None, ('req', 'patch')), parts along dimension 1, may hold values from 0 to 95
- counts: int32 [32], P('req'), parts along dimension 0, may hold values from 1 to 48, 384 in all
- timestep: int32 [2], P('req'), parts along dimension 0, may hold values from 0 to 999
- time_in: bfloat16 [256, 1152], replicated, may hold values from -0.375 to 0.375
- time_out: bfloat16 [1152, 1152], P(None, 'patch'), may hold values from -0.1875 to 0.1875
- ada_weight: bfloat16 [1152, 3456], P('patch'), may hold values from -0.375 to 0.375
- qkv_weight: bfloat16 [1152, 3456], replicated, may hold values from -2 to 2, as said below
- out_weight: bfloat16 [1152, 1152], replicated, may hold values from -0.1875 to 0.1875
Outputs:
- block_out: bfloat16 [1536, 1152], P(('req', 'patch')), parts along dimension 0
The draws below stay inside these ranges and needn't reach their ends.
There are 2 independent parts, one for each index of `req`. The reference program is written for one: setup_inputs(seed, part) draws one part's arguments, and reference() takes and returns one part's arrays. A program takes and returns all parts, laid end to end along the dimension named above; an argument that names none is the same for every part. Nothing has to cross between parts.
Inputs may be any that keep to these rules, and one draw needn't show every extreme that they name: `counts`: used slots are the first ones of each block; they sum to exactly 384, and some block uses all 48. `qkv_weight`: columns are 1152 of queries, 1152 of keys, 1152 of values, each head's 72 columns side by side.
All inputs are finite; a program needn't handle non-finite values.
Results may differ from the reference program's by a relative error of at most 0.0039.
Values may be sent and summed in bfloat16 or wider, within the bound.
No kernel may reach another device: no remote copies, remote signals or barrier semaphores. Data moves between devices by JAX's collectives and lax.ppermute only.
A program may use at most 64 MiB of HBM per device.

```python
import math
import jax
import jax.numpy as jnp
import numpy as np
from jax import lax

D = 1152
HEADS = 16
HEAD_DIM = 72
FREQ = 256
TOK_DEV = 48
SLOTS = 768
VALID = 384
N_PATCH = 16


def draw_qkv_weight(key, part):
    base_values = jax.random.truncated_normal(key, -4.0, 4.0, (D, 3 * D), jnp.float32) / math.sqrt(D)
    column_kind = jnp.arange(3 * D) // D
    scaled = base_values * jnp.where(column_kind < 2, 1.3, 1.0)[None, :]
    return jnp.clip(scaled, -2.0, 2.0).astype(jnp.bfloat16)


def set_ends(values, stream_key, low, high):
    place = [jax.random.randint(jax.random.fold_in(stream_key, axis), (), 0, length) for axis, length in enumerate(values.shape)]
    widest = values.shape.index(max(values.shape))
    neighbour = place[:widest] + [(place[widest] + 1) % values.shape[widest]] + place[widest + 1:]
    return values.at[tuple(place)].set(low).at[tuple(neighbour)].set(high)


def level_of(key, shape, split, smallest, top_value):
    def one(position, blocks):
        draws = jax.random.uniform(jax.random.fold_in(jax.random.fold_in(key, 6), position), (blocks,), jnp.float32, smallest / len(split), top_value / len(split))
        return jnp.repeat(jnp.exp(draws), shape[position] // blocks).reshape((-1,) + (1,) * (len(shape) - position - 1))

    gain = one(*split[0])
    for cut in split[1:]:
        gain = gain * one(*cut)
    return gain


def length_profile(number_of, total, reach, skew):
    portions = [(1 << 20) // math.isqrt(standing ** skew) + 1 for standing in range(2, number_of + 1)]
    spare, holding = total - reach - (number_of - 1), [1] * (number_of - 1)
    while spare > 0:
        movable = [i for i in range(number_of - 1) if holding[i] < reach]
        mass, budget = sum([portions[i] for i in movable]), spare
        for i in movable:
            extra = min(reach - holding[i], max(1, budget * portions[i] // mass), spare)
            holding[i] = holding[i] + extra
            spare = spare - extra
    return np.array([reach] + holding)


def uneven_parts(key, count, total, most, skew):
    if count == 2:
        one = jax.random.randint(key, (), max(1, total - most), min(most, total - 1) + 1)
        return jnp.stack([one, total - one])
    tallies = jnp.asarray(length_profile(count, total, most, skew), jnp.int32)
    pairs = (count - 1) // 2
    donor, sink = tallies[1:1 + 2 * pairs:2], tallies[2:2 + 2 * pairs:2]
    room = jnp.minimum(donor - 1, most - sink)
    moved = jax.random.randint(jax.random.fold_in(key, 1), (pairs,), 0, 1 << 20) % (room + 1)
    tallies = tallies.at[1:1 + 2 * pairs:2].set(donor - moved).at[2:2 + 2 * pairs:2].set(sink + moved)
    return tallies[jax.random.permutation(jax.random.fold_in(key, 2), count)]


def noise(key, shape, deviation, reach, pieces=(), kind=jnp.bfloat16):
    loudness = level_of(key, shape, pieces, -0.22, 0.18) if pieces else 1.0
    drawn = jax.random.normal(key, shape, jnp.float32) * deviation * loudness
    return jnp.minimum(jnp.maximum(drawn, -reach), reach).astype(kind)


def setup_inputs(seed: int = 0, part: int = 0) -> dict:
    streams_of = jax.random.split(jax.random.key(seed), 10)
    own_keys = jax.random.split(jax.random.fold_in(streams_of[9], part), 10)
    tokens = noise(own_keys[0], (SLOTS, D), 1.0, 6.0, ((0, 16),))
    positions = set_ends(jax.random.randint(own_keys[1], (2, SLOTS), 0, 96), jax.random.fold_in(own_keys[1], 1), 0, 95).astype(jnp.int32)
    counts = uneven_parts(own_keys[2], N_PATCH, VALID, TOK_DEV, 2).astype(jnp.int32)
    timestep = jax.random.randint(own_keys[3], (1,), 0, 1000).astype(jnp.int32)
    time_in = noise(streams_of[4], (FREQ, D), FREQ ** -0.5, 0.375)
    time_out = noise(streams_of[5], (D, D), D ** -0.5, 0.1875, ((1, 16),))
    ada_weight = noise(streams_of[6], (D, 3 * D), (D // 4) ** -0.5, 0.375, ((0, 16),))
    qkv_weight = draw_qkv_weight(jax.random.fold_in(streams_of[9], 71), part)
    out_weight = noise(streams_of[8], (D, D), D ** -0.5, 0.1875)
    return dict(tokens=tokens, positions=positions, counts=counts, timestep=timestep, time_in=time_in, time_out=time_out, ada_weight=ada_weight, qkv_weight=qkv_weight, out_weight=out_weight)


def time_features(timestep, freq_size):
    half_size = freq_size // 2
    frequencies = jnp.exp(-math.log(10000.0) * jnp.arange(half_size, dtype=jnp.float32) / half_size)
    angles = timestep.astype(jnp.float32)[:, None] * frequencies[None, :]
    return jnp.concatenate([jnp.cos(angles), jnp.sin(angles)], axis=1).astype(jnp.bfloat16)

def position_table(positions, model_width):
    quarter = model_width // 4
    omegas = jnp.power(10000.0, -jnp.arange(quarter, dtype=jnp.float32) / quarter)
    row_angle = positions[0].astype(jnp.float32)[:, None] * omegas[None, :]
    col_angle = positions[1].astype(jnp.float32)[:, None] * omegas[None, :]
    return jnp.concatenate([jnp.sin(row_angle), jnp.cos(row_angle), jnp.sin(col_angle), jnp.cos(col_angle)], axis=1)

def reference(tokens, positions, counts, timestep, time_in, time_out, ada_weight, qkv_weight, out_weight):
    model_width = tokens.shape[1]
    slot_count = tokens.shape[0]
    per_device = slot_count // N_PATCH
    features = time_features(timestep, FREQ)
    hidden_time = jax.nn.silu(jnp.dot(features, time_in, preferred_element_type=jnp.float32)).astype(jnp.bfloat16)
    cond = jnp.dot(hidden_time, time_out, preferred_element_type=jnp.float32)
    activated = jax.nn.silu(cond).astype(jnp.bfloat16)
    modulation = jnp.dot(activated, ada_weight, preferred_element_type=jnp.float32)
    shift_mod = modulation[:, :model_width]
    scale_mod = modulation[:, model_width:2 * model_width]
    gate_mod = modulation[:, 2 * model_width:]
    x_in = tokens.astype(jnp.float32) + position_table(positions, model_width)
    mean_value = lax.optimization_barrier(jnp.mean(x_in, axis=1, keepdims=True))
    centered = x_in - mean_value
    variance = lax.optimization_barrier(jnp.mean(centered * centered, axis=1, keepdims=True))
    normed = centered * lax.rsqrt(variance + 1e-06)
    modulated = (normed * (1.0 + scale_mod) + shift_mod).astype(jnp.bfloat16)
    projections = jnp.dot(modulated, qkv_weight, preferred_element_type=jnp.float32).astype(jnp.bfloat16)
    slot_valid = (jnp.arange(per_device, dtype=jnp.int32)[None, :] < counts[:, None]).reshape(slot_count)
    key_heads = projections[:, model_width:2 * model_width].astype(jnp.float32).reshape(slot_count, HEADS, HEAD_DIM)
    value_heads = projections[:, 2 * model_width:].astype(jnp.float32).reshape(slot_count, HEADS, HEAD_DIM)
    query_blocks = projections[:, :model_width].astype(jnp.float32).reshape(N_PATCH, per_device, HEADS, HEAD_DIM)
    inv_root = 1.0 / math.sqrt(HEAD_DIM)

    def attend(query_block):
        scores = jnp.einsum('qhd,khd->hqk', query_block, key_heads, precision=lax.Precision.HIGHEST) * inv_root
        scores = jnp.where(slot_valid[None, None, :], scores, -1e+30)
        row_top = lax.optimization_barrier(jnp.max(scores, axis=2, keepdims=True))
        weights = jnp.where(slot_valid[None, None, :], jnp.exp(scores - row_top), 0.0)
        denominator = lax.optimization_barrier(jnp.sum(weights, axis=2, keepdims=True))
        rounded = lax.optimization_barrier(weights.astype(jnp.bfloat16))
        weighted = jnp.einsum('hqk,khd->qhd', rounded.astype(jnp.float32), value_heads, precision=lax.Precision.HIGHEST)
        return weighted / jnp.transpose(denominator, (1, 0, 2))
    attended = lax.map(attend, query_blocks).reshape(slot_count, model_width).astype(jnp.bfloat16)
    projected = jnp.dot(attended, out_weight, preferred_element_type=jnp.float32)
    valid_column = slot_valid.astype(jnp.float32)[:, None]
    return (x_in + gate_mod * projected * valid_column).astype(jnp.bfloat16)
```

```python
import math

import jax
import jax.numpy as jnp
from jax import lax
from jax.sharding import PartitionSpec as P

HEADS = 16


neg_large = -1e30
key_block = 512


def time_features(timestep, freq_size):
    half_size = freq_size // 2
    frequencies = jnp.exp(-math.log(10000.0) * jnp.arange(half_size, dtype=jnp.float32) / half_size)
    angles = timestep.astype(jnp.float32)[:, None] * frequencies[None, :]
    return jnp.concatenate([jnp.cos(angles), jnp.sin(angles)], axis=1).astype(jnp.bfloat16)


def position_table(positions, model_width):
    quarter = model_width // 4
    omegas = jnp.power(10000.0, -jnp.arange(quarter, dtype=jnp.float32) / quarter)
    row_angle = positions[0].astype(jnp.float32)[:, None] * omegas[None, :]
    col_angle = positions[1].astype(jnp.float32)[:, None] * omegas[None, :]
    return jnp.concatenate(
        [jnp.sin(row_angle), jnp.cos(row_angle), jnp.sin(col_angle), jnp.cos(col_angle)], axis=1
    )


def attend_update(running, query_heads, key_piece, value_piece, mask_piece, inv_root):
    row_top, denominator, weighted = running
    key_count = key_piece.shape[0]
    head_count = query_heads.shape[1]
    head_size = query_heads.shape[2]
    key_heads = key_piece.reshape(key_count, head_count, head_size)
    value_heads = value_piece.reshape(key_count, head_count, head_size)
    scores = (
        jnp.einsum("qhd,khd->hqk", query_heads, key_heads, preferred_element_type=jnp.float32)
        * inv_root
    )
    scores = jnp.where(mask_piece[None, None, :], scores, neg_large)
    new_top = jnp.maximum(row_top, jnp.max(scores, axis=2))
    weights = jnp.where(mask_piece[None, None, :], jnp.exp(scores - new_top[:, :, None]), 0.0)
    factor = jnp.exp(row_top - new_top)
    denominator = denominator * factor + jnp.sum(weights, axis=2)
    rounded = weights.astype(jnp.bfloat16)
    weighted = weighted * factor[:, :, None] + jnp.einsum(
        "hqk,khd->hqd", rounded, value_heads, preferred_element_type=jnp.float32
    )
    return (new_top, denominator, weighted)


def make_folder(query_heads, key_valid, inv_root):

    def fold_keys(running, shard_piece, start_row):
        key_piece, value_piece = shard_piece
        key_count = key_piece.shape[0]
        if key_count > 2 * key_block and key_count % key_block == 0:
            block_total = key_count // key_block

            def block_step(carried, block_items):
                return (
                    attend_update(
                        carried,
                        query_heads,
                        block_items[0],
                        block_items[1],
                        block_items[2],
                        inv_root,
                    ),
                    None,
                )

            stacked = (
                key_piece.reshape(block_total, key_block, key_piece.shape[1]),
                value_piece.reshape(block_total, key_block, value_piece.shape[1]),
                key_valid.reshape(block_total, key_block),
            )
            running, unused = lax.scan(block_step, running, stacked)
            return running
        return attend_update(running, query_heads, key_piece, value_piece, key_valid, inv_root)

    return fold_keys


def initial_state(query_rows, head_count, head_size):
    return (
        jnp.full((head_count, query_rows), neg_large, jnp.float32),
        jnp.zeros((head_count, query_rows), jnp.float32),
        jnp.zeros((head_count, query_rows, head_size), jnp.float32),
    )


def finish_state(running):
    row_top, denominator, weighted = running
    normalized = weighted / denominator[:, :, None]
    head_count, query_rows, head_size = normalized.shape
    return (
        jnp.transpose(normalized, (1, 0, 2))
        .reshape(query_rows, head_count * head_size)
        .astype(jnp.bfloat16)
    )


def butterfly_sum(value, axis):
    devices = lax.axis_size(axis)
    if devices & (devices - 1):
        return lax.psum(value, axis)
    step = 1
    while step < devices:
        pairs = [(index, index ^ step) for index in range(devices)]
        value = value + lax.ppermute(value, axis, pairs)
        step *= 2
    return value


def per_device(
    tokens, positions, counts, timestep, time_in, time_out, ada_weight, qkv_weight, out_weight
):
    devices = lax.axis_size("patch")
    my_index = lax.axis_index("patch")
    local_rows = tokens.shape[0]
    model_width = tokens.shape[1]
    head_count = HEADS
    head_size = model_width // head_count
    inv_root = 1.0 / math.sqrt(head_size)
    features = time_features(timestep, time_in.shape[0])
    hidden_time = jax.nn.silu(
        jnp.dot(features, time_in, preferred_element_type=jnp.float32)
    ).astype(jnp.bfloat16)
    cond_part = jnp.dot(hidden_time, time_out, preferred_element_type=jnp.float32)
    activated = jax.nn.silu(cond_part).astype(jnp.bfloat16)
    partial_mod = jnp.dot(activated, ada_weight, preferred_element_type=jnp.float32)
    modulation = butterfly_sum(partial_mod, "patch")
    shift_mod = modulation[:, :model_width]
    scale_mod = modulation[:, model_width : 2 * model_width]
    gate_mod = modulation[:, 2 * model_width :]
    x_in = tokens.astype(jnp.float32) + position_table(positions, model_width)
    mean_value = jnp.mean(x_in, axis=1, keepdims=True)
    centered = x_in - mean_value
    variance = jnp.mean(centered * centered, axis=1, keepdims=True)
    normed = centered * lax.rsqrt(variance + 1e-06)
    modulated = (normed * (1.0 + scale_mod) + shift_mod).astype(jnp.bfloat16)
    counts_here = lax.dynamic_index_in_dim(counts, my_index, keepdims=False)
    row_ids = jnp.arange(local_rows, dtype=jnp.int32)
    row_valid = row_ids < counts_here
    projections = jnp.dot(modulated, qkv_weight, preferred_element_type=jnp.float32).astype(
        jnp.bfloat16
    )
    groups = devices // head_count
    part_rows = local_rows // groups
    query_split = projections[:, :model_width].reshape(groups, part_rows, head_count, head_size)
    query_send = jnp.transpose(query_split, (0, 2, 1, 3)).reshape(devices, part_rows, head_size)
    key_split = projections[:, model_width : 2 * model_width].reshape(
        local_rows, head_count, head_size
    )
    value_split = projections[:, 2 * model_width :].reshape(local_rows, head_count, head_size)
    pair_heads = jnp.transpose(jnp.concatenate([key_split, value_split], axis=2), (1, 0, 2))
    pair_send = jnp.broadcast_to(pair_heads[None], (groups, head_count, local_rows, 2 * head_size))
    pair_send = pair_send.reshape(devices, local_rows, 2 * head_size)
    got_query, got_pair = (
        lax.all_to_all(query_send, "patch", split_axis=0, concat_axis=0, tiled=True),
        lax.all_to_all(pair_send, "patch", split_axis=0, concat_axis=0, tiled=True),
    )
    query_rows = devices * part_rows
    query_heads = got_query.reshape(query_rows, 1, head_size)
    all_pairs = got_pair.reshape(devices * local_rows, 2 * head_size)
    key_valid = (jnp.arange(local_rows, dtype=jnp.int32)[None, :] < counts[:, None]).reshape(-1)
    folder = make_folder(query_heads, key_valid, inv_root)
    running = folder(
        initial_state(query_rows, 1, head_size),
        (all_pairs[:, :head_size], all_pairs[:, head_size:]),
        0,
    )
    head_result = finish_state(running).reshape(devices, part_rows, head_size)
    came_back = lax.all_to_all(head_result, "patch", split_axis=0, concat_axis=0, tiled=True)
    attended = jnp.transpose(
        came_back.reshape(groups, head_count, part_rows, head_size), (0, 2, 1, 3)
    )
    attended = attended.reshape(local_rows, model_width)
    projected = jnp.dot(attended, out_weight, preferred_element_type=jnp.float32)
    valid_column = row_valid.astype(jnp.float32)[:, None]
    return (x_in + gate_mod * projected * valid_column).astype(jnp.bfloat16)


def solution(mesh):
    placed = (
        P(("req", "patch"), None),
        P(None, ("req", "patch")),
        P("req"),
        P("req"),
        P(),
        P(None, "patch"),
        P("patch", None),
        P(),
        P(),
    )
    return jax.shard_map(
        per_device, mesh=mesh, in_specs=placed, out_specs=P(("req", "patch"), None), check_vma=False
    )
```

```python
import functools
import math

import jax
import jax.numpy as jnp
import numpy as np
from jax import lax
from jax.experimental import pallas as pl
from jax.experimental.pallas import tpu as pltpu
from jax.sharding import PartitionSpec as P

HEADS = 16
LANES = 128
SUM_ROWS = 8
CORE_MASK = 1
MERGE_MASK = 2
DIRECT_LIMIT = 16
neg_large = -1e30


def vmem():
    return pl.BlockSpec(memory_space=pltpu.VMEM)


def smem():
    return pl.BlockSpec(memory_space=pltpu.SMEM)


def lane_table(model_width, freq_size):
    quarter = model_width // 4
    half = freq_size // 2
    lane = np.arange(model_width)
    table = np.zeros((SUM_ROWS, model_width), np.float32)
    table[0] = np.power(10000.0, -(lane % quarter) / quarter)
    table[1] = (lane // quarter) % 2
    table[2] = lane // (2 * quarter)
    feature = np.arange(freq_size)
    table[3, :freq_size] = np.exp(-math.log(10000.0) * (feature % half) / half)
    table[4, :freq_size] = feature < half
    return table


def sine(angle, shifted):
    turns = jnp.floor(angle * (0.5 / math.pi) + 0.5)
    rest = angle - turns * 6.28125
    rest = rest - turns * (2.0 * math.pi - 6.28125)
    rest = rest + shifted * (0.5 * math.pi)
    rest = jnp.where(rest > 0.5 * math.pi, math.pi - rest, rest)
    rest = jnp.where(rest < -0.5 * math.pi, -math.pi - rest, rest)
    square = rest * rest
    series = 1.0 / math.factorial(13)
    for power in (11, 9, 7, 5, 3, 1):
        sign = -1.0 if power % 4 == 3 else 1.0
        series = series * square + sign / math.factorial(power)
    return rest * series


def silu(value):
    return value / (1.0 + jnp.exp(-value))


def high_low(value):
    high = value.astype(jnp.bfloat16)
    return high, (value - high.astype(jnp.float32)).astype(jnp.bfloat16)


def front_kernel(
    timestep, tokens, positions, table, time_in, time_out, ada_weight, message, sums, x_in_ref
):
    rows, width = tokens.shape
    freq_size = time_in.shape[0]
    angle = timestep[0].astype(jnp.float32) * jnp.broadcast_to(
        table[3:4, :freq_size], (SUM_ROWS, freq_size)
    )
    shifted = jnp.broadcast_to(table[4:5, :freq_size], (SUM_ROWS, freq_size))
    features = sine(angle, shifted).astype(jnp.bfloat16)
    hidden = silu(jnp.dot(features, time_in[...], preferred_element_type=jnp.float32))
    cond = jnp.dot(
        hidden.astype(jnp.bfloat16), time_out[...], preferred_element_type=jnp.float32
    )
    partial = jnp.dot(
        silu(cond).astype(jnp.bfloat16), ada_weight[...], preferred_element_type=jnp.float32
    )
    row_id = lax.broadcasted_iota(jnp.int32, (SUM_ROWS, width), 0)
    packed = jnp.zeros((SUM_ROWS, width), jnp.float32)
    for piece in range(3):
        high, low = high_low(partial[:, piece * width : (piece + 1) * width])
        packed = jnp.where(row_id == 2 * piece, high.astype(jnp.float32), packed)
        packed = jnp.where(row_id == 2 * piece + 1, low.astype(jnp.float32), packed)
    packed = packed.astype(jnp.bfloat16)
    sums[...] = packed
    message[rows:, :] = packed

    place = positions[...].astype(jnp.float32)
    same = lax.broadcasted_iota(jnp.int32, (rows, rows), 0) == lax.broadcasted_iota(
        jnp.int32, (rows, rows), 1
    )
    column = [
        jnp.sum(jnp.where(same, place[axis : axis + 1, :], 0.0), axis=1, keepdims=True)
        for axis in range(2)
    ]
    where_to = jnp.where(table[2:3, :] > 0.5, column[1], column[0])
    x_in = tokens[...].astype(jnp.float32) + sine(where_to * table[0:1, :], table[1:2, :])
    x_in_ref[...] = x_in
    centered = x_in - jnp.mean(x_in, axis=1, keepdims=True)
    variance = jnp.mean(centered * centered, axis=1, keepdims=True)
    message[:rows, :] = (centered * lax.rsqrt(variance + 1e-06)).astype(jnp.bfloat16)


def unpack_sums(packed):
    width = packed.shape[1]
    value = packed.astype(jnp.float32)
    row_id = lax.broadcasted_iota(jnp.int32, (SUM_ROWS, width), 0)
    out = jnp.zeros((SUM_ROWS, width), jnp.float32)
    for piece in range(3):
        both = value[2 * piece : 2 * piece + 1, :] + value[2 * piece + 1 : 2 * piece + 2, :]
        out = jnp.where(row_id == piece, both, out)
    return out


def add_kernel(*refs):
    out = refs[-1]
    total = None
    for ref in refs[:-1]:
        rows = ref.shape[0]
        value = ref[rows - SUM_ROWS :, :].astype(jnp.float32)
        total = value if total is None else total + value
    out[...] = unpack_sums(total)


def attend_kernel(part_index, parts, block_rows, key_count, *refs):
    counts, sums_a, sums_b = refs[:3]
    key_refs = refs[3 : 3 + key_count]
    query_refs = refs[3 + key_count : 7 + key_count]
    weight = refs[7 + key_count]
    near_out, near_lse, far_out, far_lse = refs[8 + key_count : 12 + key_count]
    mod_keys, mod_queries, keys, values, queries = refs[12 + key_count :]
    width = weight.shape[0]
    head_size = width // HEADS
    my_index = lax.axis_index("patch")
    sums = sums_a[...] + sums_b[...]
    shift = sums[0:1, :]
    scale = 1.0 + sums[1:2, :]

    def modulate(value):
        return (value.astype(jnp.float32) * scale + shift).astype(jnp.bfloat16)

    place = 0
    for ref in key_refs:
        for start in range(0, ref.shape[0], block_rows + SUM_ROWS):
            mod_keys[place : place + block_rows, :] = modulate(ref[start : start + block_rows, :])
            place += block_rows
    for index, ref in enumerate(query_refs):
        mod_queries[index * block_rows : (index + 1) * block_rows, :] = modulate(
            ref[:block_rows, :]
        )
    piece = 3 * LANES
    for start in range(0, width, piece):
        stop = min(start + piece, width)
        queries[:, start:stop] = jnp.dot(
            mod_queries[...], weight[:, start:stop], preferred_element_type=jnp.float32
        ).astype(jnp.bfloat16)
        keys[:, start:stop] = jnp.dot(
            mod_keys[...], weight[:, width + start : width + stop], preferred_element_type=jnp.float32
        ).astype(jnp.bfloat16)
        values[:, start:stop] = jnp.dot(
            mod_keys[...],
            weight[:, 2 * width + start : 2 * width + stop],
            preferred_element_type=jnp.float32,
        ).astype(jnp.bfloat16)

    total_keys = keys.shape[0]
    total_queries = queries.shape[0]
    key_id = lax.broadcasted_iota(jnp.int32, (1, total_keys), 1)
    valid = key_id < 0
    for block in range(parts):
        used = counts[part_index(my_index, block)]
        first = block * block_rows
        valid = jnp.logical_or(
            valid, jnp.logical_and(key_id >= first, key_id < first + used)
        )
    inv_root = 1.0 / math.sqrt(head_size)
    lse_lane = lax.broadcasted_iota(jnp.int32, (total_queries, LANES), 1)
    lse_all = jnp.zeros((total_queries, LANES), jnp.float32)
    half = total_queries // 2
    for head in range(HEADS):
        low, high = head * head_size, (head + 1) * head_size
        first, last = low // LANES * LANES, -(-high // LANES) * LANES
        lane = lax.broadcasted_iota(jnp.int32, (1, last - first), 1) + first
        inside = jnp.logical_and(lane >= low, lane < high)
        query = jnp.where(inside, queries[:, first:last], jnp.zeros((), jnp.bfloat16))
        scores = lax.dot_general(
            query,
            keys[:, first:last],
            (((1,), (1,)), ((), ())),
            preferred_element_type=jnp.float32,
        )
        scores = jnp.where(valid, scores * inv_root, neg_large)
        top = jnp.max(scores, axis=1, keepdims=True)
        weights = jnp.where(valid, jnp.exp(scores - top), 0.0)
        total = jnp.sum(weights, axis=1, keepdims=True)
        result = jnp.dot(
            weights.astype(jnp.bfloat16), values[:, first:last], preferred_element_type=jnp.float32
        )
        result = (result / total).astype(jnp.bfloat16)
        lse_all = jnp.where(lse_lane == head, top + jnp.log(total), lse_all)
        for out, start in ((near_out, 0), (far_out, half)):
            chosen = result[start : start + half, :]
            if low > first:
                chosen = jnp.where(inside, chosen, out[:, first:last])
            out[:, first:last] = chosen
    near_lse[...] = lse_all[:half, :]
    far_lse[...] = lse_all[half:, :]


def spread(value, width):
    head_size = width // HEADS
    head_id = lax.broadcasted_iota(jnp.int32, (LANES, width), 0)
    lane_id = lax.broadcasted_iota(jnp.int32, (LANES, width), 1)
    low = head_id * head_size
    expand = jnp.logical_and(lane_id >= low, lane_id < low + head_size).astype(jnp.bfloat16)
    high, rest = high_low(value)
    return jnp.dot(high, expand, preferred_element_type=jnp.float32) + jnp.dot(
        rest, expand, preferred_element_type=jnp.float32
    )


def merge(value_a, lse_a, value_b, lse_b):
    top = jnp.maximum(lse_a, lse_b)
    part_a = jnp.exp(lse_a - top)
    part_b = jnp.exp(lse_b - top)
    total = part_a + part_b
    share = spread(part_b / total, value_a.shape[1])
    first = value_a.astype(jnp.float32)
    value = first + share * (value_b.astype(jnp.float32) - first)
    return value, top + jnp.log(total)


def merge_kernel(value_a, lse_a, value_b, lse_b, own_out, own_lse, send_out, send_lse):
    value, lse = merge(value_a[...], lse_a[...], value_b[...], lse_b[...])
    rows = own_out.shape[0]
    value = value.astype(jnp.bfloat16)
    own_out[...] = value[:rows, :]
    own_lse[...] = lse[:rows, :]
    send_out[...] = value[rows:, :]
    send_lse[...] = lse[rows:, :]


def finish_kernel(
    counts, value_a, lse_a, value_b, lse_b, x_in, sums_a, sums_b, weight, out
):
    value, _ = merge(value_a[...], lse_a[...], value_b[...], lse_b[...])
    used = counts[lax.axis_index("patch")]
    gate = sums_a[2:3, :] + sums_b[2:3, :]
    projected = jnp.dot(
        value.astype(jnp.bfloat16), weight[...], preferred_element_type=jnp.float32
    )
    row_id = lax.broadcasted_iota(jnp.int32, projected.shape, 0)
    valid = (row_id < used).astype(jnp.float32)
    out[...] = (x_in[...] + gate * projected * valid).astype(jnp.bfloat16)


def per_device(
    tokens, positions, counts, timestep, time_in, time_out, ada_weight, qkv_weight, out_weight
):
    devices = lax.axis_size("patch")
    rows, width = tokens.shape
    shape = jax.ShapeDtypeStruct
    table = jnp.asarray(lane_table(width, time_in.shape[0]))

    def swap(value, mask):
        pairs = [(index, index ^ mask) for index in range(devices)]
        return lax.ppermute(value, "patch", pairs)

    message, sums, x_in = pl.pallas_call(
        front_kernel,
        out_shape=(
            shape((rows + SUM_ROWS, width), jnp.bfloat16),
            shape((SUM_ROWS, width), jnp.bfloat16),
            shape((rows, width), jnp.float32),
        ),
        in_specs=[smem()] + [vmem()] * 6,
        out_specs=(vmem(),) * 3,
        name="front",
    )(timestep, tokens, positions, table, time_in, time_out, ada_weight)

    key_masks = [mask for mask in range(devices) if not mask & (CORE_MASK | MERGE_MASK)]
    if devices <= DIRECT_LIMIT:
        got = {mask: swap(message, mask) for mask in [*key_masks[1:], MERGE_MASK]}
        others = [mask | MERGE_MASK for mask in key_masks[1:]]
        got_sums = [swap(sums, mask) for mask in others]
        key_parts = [message] + [got[mask] for mask in key_masks[1:]]
        across = got[MERGE_MASK]

        def part_index(my_index, block):
            return jnp.bitwise_xor(my_index, key_masks[block])

        half_sums = pl.pallas_call(
            add_kernel,
            out_shape=shape((SUM_ROWS, width), jnp.float32),
            in_specs=[vmem()] * (1 + len(got) + len(got_sums)),
            out_specs=vmem(),
            name="add",
        )(sums, *got.values(), *got_sums)
    else:
        across = swap(message, MERGE_MASK)
        spread_mask = CORE_MASK | MERGE_MASK
        groups = [
            [mask | rest for mask in key_masks] for rest in range(spread_mask + 1)
        ]
        key_parts = [lax.all_gather(message, "patch", axis_index_groups=groups, tiled=True)]
        running = sums.astype(jnp.float32)
        step = MERGE_MASK
        while step < devices:
            running = running + swap(running, step)
            step *= 2
        half_sums = pl.pallas_call(
            add_kernel,
            out_shape=shape((SUM_ROWS, width), jnp.float32),
            in_specs=[vmem()],
            out_specs=vmem(),
            name="add",
        )(running)

        def part_index(my_index, block):
            return jnp.bitwise_and(my_index, spread_mask) + key_masks[block]

    other_sums = swap(half_sums, CORE_MASK)
    other_own = swap(message, CORE_MASK)
    other_across = swap(across, CORE_MASK)

    total_keys = rows * len(key_masks)
    total_queries = 4 * rows
    half = total_queries // 2
    near, near_lse, far, far_lse = pl.pallas_call(
        functools.partial(attend_kernel, part_index, len(key_masks), rows, len(key_parts)),
        out_shape=(
            shape((half, width), jnp.bfloat16),
            shape((half, LANES), jnp.float32),
            shape((half, width), jnp.bfloat16),
            shape((half, LANES), jnp.float32),
        ),
        in_specs=[smem()] + [vmem()] * (7 + len(key_parts)),
        out_specs=(vmem(),) * 4,
        scratch_shapes=[
            pltpu.VMEM((total_keys, width), jnp.bfloat16),
            pltpu.VMEM((total_queries, width), jnp.bfloat16),
            pltpu.VMEM((total_keys, width), jnp.bfloat16),
            pltpu.VMEM((total_keys, width), jnp.bfloat16),
            pltpu.VMEM((total_queries, width), jnp.bfloat16),
        ],
        name="attend",
    )(
        counts,
        half_sums,
        other_sums,
        *key_parts,
        message,
        across,
        other_own,
        other_across,
        qkv_weight,
    )
    back, back_lse = swap(far, CORE_MASK), swap(far_lse, CORE_MASK)
    own, own_lse, send, send_lse = pl.pallas_call(
        merge_kernel,
        out_shape=(
            shape((rows, width), jnp.bfloat16),
            shape((rows, LANES), jnp.float32),
            shape((rows, width), jnp.bfloat16),
            shape((rows, LANES), jnp.float32),
        ),
        in_specs=[vmem()] * 4,
        out_specs=(vmem(),) * 4,
        name="merge",
    )(near, near_lse, back, back_lse)
    last, last_lse = swap(send, MERGE_MASK), swap(send_lse, MERGE_MASK)
    return pl.pallas_call(
        finish_kernel,
        out_shape=shape((rows, width), jnp.bfloat16),
        in_specs=[smem()] + [vmem()] * 8,
        out_specs=vmem(),
        name="finish",
    )(counts, own, own_lse, last, last_lse, x_in, half_sums, other_sums, out_weight)


def solution(mesh):
    placed = (
        P(("req", "patch"), None),
        P(None, ("req", "patch")),
        P("req"),
        P("req"),
        P(),
        P(None, "patch"),
        P("patch", None),
        P(),
        P(),
    )
    return jax.shard_map(
        per_device, mesh=mesh, in_specs=placed, out_specs=P(("req", "patch"), None), check_vma=False
    )
```

```python
import functools
import math

import jax
import jax.numpy as jnp
import numpy as np
from jax import lax
from jax.experimental import pallas as pl
from jax.experimental.pallas import tpu as pltpu
from jax.sharding import PartitionSpec as P


HEADS = 16
LANES = 128
SUM_ROWS = 8
CORE_MASK = 1
MERGE_MASK = 2
DIRECT_LIMIT = 16
neg_large = -1e30


def grant(mebibytes):
    return pltpu.CompilerParams(vmem_limit_bytes=mebibytes << 20)


def vmem():
    return pl.BlockSpec(memory_space=pltpu.VMEM)


def lane_table(model_width, freq_size):
    quarter = model_width // 4
    half = freq_size // 2
    lane = np.arange(model_width)
    table = np.zeros((SUM_ROWS, model_width), np.float32)
    table[0] = np.power(10000.0, -(lane % quarter) / quarter)
    table[1] = (lane // quarter) % 2
    table[2] = lane // (2 * quarter)
    feature = np.arange(freq_size)
    table[3, :freq_size] = np.exp(-math.log(10000.0) * (feature % half) / half)
    table[4, :freq_size] = feature < half
    return table


def sine(angle, shifted):
    turns = jnp.floor(angle * (0.5 / math.pi) + 0.5)
    rest = angle - turns * 6.28125
    rest = rest - turns * (2.0 * math.pi - 6.28125)
    rest = rest + shifted * (0.5 * math.pi)
    rest = jnp.where(rest > 0.5 * math.pi, math.pi - rest, rest)
    rest = jnp.where(rest < -0.5 * math.pi, -math.pi - rest, rest)
    square = rest * rest
    series = 1.0 / math.factorial(13)
    for power in (11, 9, 7, 5, 3, 1):
        sign = -1.0 if power % 4 == 3 else 1.0
        series = series * square + sign / math.factorial(power)
    return rest * series


def silu(value):
    return value / (1.0 + jnp.exp(-value))


def high_low(value):
    high = value.astype(jnp.bfloat16)
    return high, (value - high.astype(jnp.float32)).astype(jnp.bfloat16)


def front_kernel(
    part_index,
    parts,
    timestep,
    counts_far,
    tokens_far,
    positions_far,
    table_far,
    time_in_far,
    time_out_far,
    ada_weight_far,
    message,
    sums,
    x_in_ref,
    bias,
    row_valid,
    counts,
    tokens,
    positions,
    table,
    time_in,
    time_out,
    ada_weight,
    arrived,
):
    order = (
        (table_far, table),
        (time_in_far, time_in),
        (time_out_far, time_out),
        (ada_weight_far, ada_weight),
        (positions_far, positions),
        (tokens_far, tokens),
        (counts_far, counts),
    )
    copies = [
        pltpu.make_async_copy(far, near, arrived.at[index])
        for index, (far, near) in enumerate(order)
    ]
    for copy in copies:
        copy.start()
    rows, width = tokens.shape
    freq_size = time_in.shape[0]
    copies[0].wait()
    angle = timestep[0].astype(jnp.float32) * jnp.broadcast_to(
        table[3:4, :freq_size], (SUM_ROWS, freq_size)
    )
    shifted = jnp.broadcast_to(table[4:5, :freq_size], (SUM_ROWS, freq_size))
    features = sine(angle, shifted).astype(jnp.bfloat16)
    copies[1].wait()
    hidden = silu(jnp.dot(features, time_in[...], preferred_element_type=jnp.float32))
    copies[2].wait()
    cond = lax.dot_general(
        hidden.astype(jnp.bfloat16),
        time_out[...],
        (((1,), (1,)), ((), ())),
        preferred_element_type=jnp.float32,
    )
    copies[3].wait()
    partial = jnp.dot(
        silu(cond).astype(jnp.bfloat16), ada_weight[...], preferred_element_type=jnp.float32
    )
    row_id = lax.broadcasted_iota(jnp.int32, (SUM_ROWS, width), 0)
    packed = jnp.zeros((SUM_ROWS, width), jnp.float32)
    for piece in range(3):
        high, low = high_low(partial[:, piece * width : (piece + 1) * width])
        packed = jnp.where(row_id == 2 * piece, high.astype(jnp.float32), packed)
        packed = jnp.where(row_id == 2 * piece + 1, low.astype(jnp.float32), packed)
    packed = packed.astype(jnp.bfloat16)
    sums[...] = packed
    message[rows:, :] = packed

    copies[4].wait()
    place = positions[...].astype(jnp.float32)
    same = lax.broadcasted_iota(jnp.int32, (rows, rows), 0) == lax.broadcasted_iota(
        jnp.int32, (rows, rows), 1
    )
    column = [
        jnp.sum(jnp.where(same, place[axis : axis + 1, :], 0.0), axis=1, keepdims=True)
        for axis in range(2)
    ]
    where_to = jnp.where(table[2:3, :] > 0.5, column[1], column[0])
    embed = sine(where_to * table[0:1, :], table[1:2, :])
    copies[5].wait()
    x_in = tokens[...].astype(jnp.float32) + embed
    x_in_ref[...] = x_in
    centered = x_in - jnp.mean(x_in, axis=1, keepdims=True)
    variance = jnp.mean(centered * centered, axis=1, keepdims=True)
    message[:rows, :] = (centered * lax.rsqrt(variance + 1e-06)).astype(jnp.bfloat16)

    copies[6].wait()
    my_index = lax.axis_index("patch")
    key_id = lax.broadcasted_iota(jnp.int32, bias.shape, 1)
    valid = key_id < 0
    for block in range(parts):
        first = block * rows
        used = counts[part_index(my_index, block)]
        valid = jnp.logical_or(valid, jnp.logical_and(key_id >= first, key_id < first + used))
    bias[...] = jnp.where(valid, 0.0, neg_large)
    own_row = lax.broadcasted_iota(jnp.int32, row_valid.shape, 0)
    row_valid[...] = (own_row < counts[my_index]).astype(jnp.float32)


def load_kernel(after, weight_far, weight, arrived):
    pieces = arrived.shape[0]
    size = weight.shape[0] // pieces
    copies = [
        pltpu.make_async_copy(
            weight_far.at[pl.ds(index * size, size)],
            weight.at[pl.ds(index * size, size)],
            arrived.at[index],
        )
        for index in range(pieces)
    ]
    for copy in copies:
        copy.start()
    for copy in copies:
        copy.wait()


def unpack_sums(packed):
    width = packed.shape[1]
    value = packed.astype(jnp.float32)
    row_id = lax.broadcasted_iota(jnp.int32, (SUM_ROWS, width), 0)
    out = jnp.zeros((SUM_ROWS, width), jnp.float32)
    for piece in range(3):
        both = value[2 * piece : 2 * piece + 1, :] + value[2 * piece + 1 : 2 * piece + 2, :]
        out = jnp.where(row_id == piece, both, out)
    return out


def add_kernel(*refs):
    out = refs[-1]
    total = None
    for ref in refs[:-1]:
        rows = ref.shape[0]
        value = ref[rows - SUM_ROWS :, :].astype(jnp.float32)
        total = value if total is None else total + value
    out[...] = unpack_sums(total)


def attend_kernel(block_rows, key_count, *refs):
    bias, sums_a, sums_b = refs[:3]
    key_refs = refs[3 : 3 + key_count]
    query_refs = refs[3 + key_count : 7 + key_count]
    weight = refs[7 + key_count]
    near_out, far_out = refs[8 + key_count : 10 + key_count]
    mod_keys, mod_queries, keys, values, queries = refs[10 + key_count :]
    width = weight.shape[0]
    head_size = width // HEADS
    sums = sums_a[...] + sums_b[...]
    shift = sums[0:1, :]
    scale = 1.0 + sums[1:2, :]

    def modulate(value):
        return (value.astype(jnp.float32) * scale + shift).astype(jnp.bfloat16)

    place = 0
    for ref in key_refs:
        for start in range(0, ref.shape[0], block_rows + SUM_ROWS):
            mod_keys[place : place + block_rows, :] = modulate(ref[start : start + block_rows, :])
            place += block_rows
    for index, ref in enumerate(query_refs):
        mod_queries[index * block_rows : (index + 1) * block_rows, :] = modulate(
            ref[:block_rows, :]
        )
    piece = 3 * LANES
    for start in range(0, width, piece):
        stop = min(start + piece, width)
        queries[:, start:stop] = jnp.dot(
            mod_queries[...], weight[:, start:stop], preferred_element_type=jnp.float32
        ).astype(jnp.bfloat16)
        keys[:, start:stop] = jnp.dot(
            mod_keys[...], weight[:, width + start : width + stop], preferred_element_type=jnp.float32
        ).astype(jnp.bfloat16)
        values[:, start:stop] = jnp.dot(
            mod_keys[...],
            weight[:, 2 * width + start : 2 * width + stop],
            preferred_element_type=jnp.float32,
        ).astype(jnp.bfloat16)

    total_queries = queries.shape[0]
    half = total_queries // 2
    base_two = math.log2(math.e) / math.sqrt(head_size)
    lse_lane = lax.broadcasted_iota(jnp.int32, (total_queries, LANES), 1)
    lse_all = jnp.zeros((total_queries, LANES), jnp.float32)
    key_bias = bias[0:1, :]
    held = None
    for head in range(HEADS):
        low, high = head * head_size, (head + 1) * head_size
        first, last = low // LANES * LANES, -(-high // LANES) * LANES
        lane = lax.broadcasted_iota(jnp.int32, (1, last - first), 1) + first
        inside = jnp.logical_and(lane >= low, lane < high)
        query = jnp.where(inside, queries[:, first:last], jnp.zeros((), jnp.bfloat16))
        scores = lax.dot_general(
            query,
            keys[:, first:last],
            (((1,), (1,)), ((), ())),
            preferred_element_type=jnp.float32,
        )
        scores = scores + key_bias
        top = jnp.max(scores, axis=1, keepdims=True)
        weights = jnp.exp2((scores - top) * base_two)
        total = jnp.sum(weights, axis=1, keepdims=True)
        result = jnp.dot(
            weights.astype(jnp.bfloat16), values[:, first:last], preferred_element_type=jnp.float32
        )
        result = result * (1.0 / total)
        lse_all = jnp.where(lse_lane == head, top * base_two + jnp.log2(total), lse_all)
        for start in range(first, last, LANES):
            tile = result[:, start - first : start - first + LANES]
            if start < low:
                tile = jnp.where(inside[:, start - first : start - first + LANES], tile, held)
            if start + LANES <= high:
                tile = tile.astype(jnp.bfloat16)
                near_out[:, start : start + LANES] = tile[:half, :]
                far_out[:, start : start + LANES] = tile[half:, :]
            else:
                held = tile
    packed = pack_lse(lse_all)
    near_out[:, width:] = packed[:half, :]
    far_out[:, width:] = packed[half:, :]


def pack_lse(lse):
    high = lse.astype(jnp.bfloat16).astype(jnp.float32)
    middle = (lse - high).astype(jnp.bfloat16).astype(jnp.float32)
    low = lse - high - middle
    return (high + pltpu.roll(middle, HEADS, 1) + pltpu.roll(low, 2 * HEADS, 1)).astype(
        jnp.bfloat16
    )


def unpack_lse(packed):
    source = lax.broadcasted_iota(jnp.int32, (LANES, LANES), 0)
    target = lax.broadcasted_iota(jnp.int32, (LANES, LANES), 1)
    chosen = source == target
    for piece in range(1, 3):
        chosen = jnp.logical_or(chosen, source == target + piece * HEADS)
    chosen = jnp.logical_and(chosen, target < HEADS).astype(jnp.bfloat16)
    return jnp.dot(packed, chosen, preferred_element_type=jnp.float32)


def spread(value, width):
    head_size = width // HEADS
    head_id = lax.broadcasted_iota(jnp.int32, (LANES, width), 0)
    lane_id = lax.broadcasted_iota(jnp.int32, (LANES, width), 1)
    low = head_id * head_size
    expand = jnp.logical_and(lane_id >= low, lane_id < low + head_size).astype(jnp.bfloat16)
    high, rest = high_low(value)
    return jnp.dot(high, expand, preferred_element_type=jnp.float32) + jnp.dot(
        rest, expand, preferred_element_type=jnp.float32
    )


def merge(packed_a, packed_b):
    width = packed_a.shape[1] - LANES
    lse_a, lse_b = unpack_lse(packed_a[:, width:]), unpack_lse(packed_b[:, width:])
    top = jnp.maximum(lse_a, lse_b)
    part_a = jnp.exp2(lse_a - top)
    part_b = jnp.exp2(lse_b - top)
    total = part_a + part_b
    share = spread(part_b / total, width)
    first = packed_a[:, :width].astype(jnp.float32)
    value = first + share * (packed_b[:, :width].astype(jnp.float32) - first)
    return value, top + jnp.log2(total)


def merge_kernel(packed_a, packed_b, own_out, send_out):
    value, lse = merge(packed_a[...], packed_b[...])
    rows, width = own_out.shape[0], value.shape[1]
    value = value.astype(jnp.bfloat16)
    lane = lax.broadcasted_iota(jnp.int32, lse.shape, 1)
    packed = pack_lse(jnp.where(lane < HEADS, lse, 0.0))
    own_out[:, :width] = value[:rows, :]
    own_out[:, width:] = packed[:rows, :]
    send_out[:, :width] = value[rows:, :]
    send_out[:, width:] = packed[rows:, :]


def finish_kernel(packed_a, packed_b, x_in, row_valid, sums_a, sums_b, weight, out):
    value, _ = merge(packed_a[...], packed_b[...])
    gate = sums_a[2:3, :] + sums_b[2:3, :]
    projected = jnp.dot(
        value.astype(jnp.bfloat16), weight[...], preferred_element_type=jnp.float32
    )
    out[...] = (x_in[...] + gate * projected * row_valid[:, 0:1]).astype(jnp.bfloat16)


def far():
    return pl.BlockSpec(memory_space=pltpu.HBM)


def stay_far(array):
    return pltpu.with_memory_space_constraint(array, pltpu.HBM)


def per_device(
    tokens, positions, counts, timestep, time_in, time_out, ada_weight, qkv_weight, out_weight
):
    devices = lax.axis_size("patch")
    rows, width = tokens.shape
    shape = jax.ShapeDtypeStruct
    table = jnp.asarray(lane_table(width, time_in.shape[0]))
    key_masks = [mask for mask in range(devices) if not mask & (CORE_MASK | MERGE_MASK)]
    direct = devices <= DIRECT_LIMIT

    def swap(value, mask):
        pairs = [(index, index ^ mask) for index in range(devices)]
        return lax.ppermute(value, "patch", pairs)

    def part_index(my_index, block):
        if direct:
            return jnp.bitwise_xor(my_index, key_masks[block])
        return jnp.bitwise_and(my_index, CORE_MASK | MERGE_MASK) + key_masks[block]

    inputs = (timestep, counts, tokens, positions, table, time_in, time_out.T, ada_weight)
    message, sums, x_in, bias, row_valid = pl.pallas_call(
        functools.partial(front_kernel, part_index, len(key_masks)),
        out_shape=(
            shape((rows + SUM_ROWS, width), jnp.bfloat16),
            shape((SUM_ROWS, width), jnp.bfloat16),
            shape((rows, width), jnp.float32),
            shape((SUM_ROWS, rows * len(key_masks)), jnp.float32),
            shape((rows, LANES), jnp.float32),
        ),
        in_specs=[pl.BlockSpec(memory_space=pltpu.SMEM)] + [far()] * (len(inputs) - 1),
        out_specs=(vmem(),) * 5,
        scratch_shapes=[
            (pltpu.SMEM if array.ndim == 1 else pltpu.VMEM)(array.shape, array.dtype)
            for array in inputs[1:]
        ]
        + [pltpu.SemaphoreType.DMA((len(inputs) - 1,))],
        compiler_params=grant(8),
        name="front",
    )(inputs[0], *[stay_far(array) for array in inputs[1:]])

    load = pl.pallas_call(
        load_kernel,
        out_shape=shape(qkv_weight.shape, qkv_weight.dtype),
        in_specs=[vmem(), far()],
        out_specs=vmem(),
        scratch_shapes=[pltpu.SemaphoreType.DMA((8,))],
        compiler_params=grant(1),
        cost_estimate=pl.CostEstimate(
            flops=1 << 32, bytes_accessed=4 * qkv_weight.size, transcendentals=0
        ),
        name="load",
    )
    weight = load(row_valid, stay_far(qkv_weight))

    if direct:
        got = {mask: swap(message, mask) for mask in [*key_masks[1:], MERGE_MASK]}
        others = [mask | MERGE_MASK for mask in key_masks[1:]]
        got_sums = [swap(sums, mask) for mask in others]
        key_parts = [message] + [got[mask] for mask in key_masks[1:]]
        across = got[MERGE_MASK]
        addends = (sums, *got.values(), *got_sums)
    else:
        across = swap(message, MERGE_MASK)
        spread_mask = CORE_MASK | MERGE_MASK
        groups = [[mask | rest for mask in key_masks] for rest in range(spread_mask + 1)]
        key_parts = [lax.all_gather(message, "patch", axis_index_groups=groups, tiled=True)]
        running = sums.astype(jnp.float32)
        step = MERGE_MASK
        while step < devices:
            running = running + swap(running, step)
            step *= 2
        addends = (running,)
    half_sums = pl.pallas_call(
        add_kernel,
        out_shape=shape((SUM_ROWS, width), jnp.float32),
        in_specs=[vmem()] * len(addends),
        out_specs=vmem(),
        compiler_params=grant(4),
        name="add",
    )(*addends)
    other_sums = swap(half_sums, CORE_MASK)
    other_own = swap(message, CORE_MASK)
    other_across = swap(across, CORE_MASK)

    total_keys = rows * len(key_masks)
    total_queries = 4 * rows
    half = total_queries // 2
    near, away = pl.pallas_call(
        functools.partial(attend_kernel, rows, len(key_parts)),
        out_shape=(shape((half, width + LANES), jnp.bfloat16),) * 2,
        in_specs=[vmem()] * (8 + len(key_parts)),
        out_specs=(vmem(),) * 2,
        scratch_shapes=[
            pltpu.VMEM((total_keys, width), jnp.bfloat16),
            pltpu.VMEM((total_queries, width), jnp.bfloat16),
            pltpu.VMEM((total_keys, width), jnp.bfloat16),
            pltpu.VMEM((total_keys, width), jnp.bfloat16),
            pltpu.VMEM((total_queries, width), jnp.bfloat16),
        ],
        compiler_params=grant(32),
        name="attend",
    )(
        bias,
        half_sums,
        other_sums,
        *key_parts,
        message,
        across,
        other_own,
        other_across,
        weight,
    )
    own, send = pl.pallas_call(
        merge_kernel,
        out_shape=(shape((rows, width + LANES), jnp.bfloat16),) * 2,
        in_specs=[vmem()] * 2,
        out_specs=(vmem(),) * 2,
        compiler_params=grant(6),
        name="merge",
    )(near, swap(away, CORE_MASK))
    return pl.pallas_call(
        finish_kernel,
        out_shape=shape((rows, width), jnp.bfloat16),
        in_specs=[vmem()] * 7,
        out_specs=vmem(),
        compiler_params=grant(8),
        name="finish",
    )(own, swap(send, MERGE_MASK), x_in, row_valid, half_sums, other_sums, out_weight)


def solution(mesh):
    placed = (
        P(("req", "patch"), None),
        P(None, ("req", "patch")),
        P("req"),
        P("req"),
        P(),
        P(None, "patch"),
        P("patch", None),
        P(),
        P(),
    )

    return jax.shard_map(
        per_device, mesh=mesh, in_specs=placed, out_specs=P(("req", "patch"), None), check_vma=False
    )
```

```python
import functools
import math

import jax
import jax.numpy as jnp
import numpy as np
from jax import lax
from jax.experimental import pallas as pl
from jax.experimental.pallas import tpu as pltpu
from jax.sharding import PartitionSpec as P


HEADS = 16
LANES = 128
SUM_ROWS = 8
CORE_MASK = 1
MERGE_MASK = 2
DIRECT_LIMIT = 16
ATTEND_GRANT = 24
neg_large = -1e30


def grant(mebibytes):
    return pltpu.CompilerParams(vmem_limit_bytes=mebibytes << 20)


def vmem():
    return pl.BlockSpec(memory_space=pltpu.VMEM)


def lane_table(model_width, freq_size):
    quarter = model_width // 4
    half = freq_size // 2
    lane = np.arange(model_width)
    table = np.zeros((SUM_ROWS, model_width), np.float32)
    table[0] = np.power(10000.0, -(lane % quarter) / quarter)
    table[1] = (lane // quarter) % 2
    table[2] = lane // (2 * quarter)
    feature = np.arange(freq_size)
    table[3, :freq_size] = np.exp(-math.log(10000.0) * (feature % half) / half)
    table[4, :freq_size] = feature < half
    return table


def sine(angle, shifted):
    turns = jnp.floor(angle * (0.5 / math.pi) + 0.5)
    rest = angle - turns * 6.28125
    rest = rest - turns * (2.0 * math.pi - 6.28125)
    rest = rest + shifted * (0.5 * math.pi)
    rest = jnp.where(rest > 0.5 * math.pi, math.pi - rest, rest)
    rest = jnp.where(rest < -0.5 * math.pi, -math.pi - rest, rest)
    square = rest * rest
    series = 1.0 / math.factorial(13)
    for power in (11, 9, 7, 5, 3, 1):
        sign = -1.0 if power % 4 == 3 else 1.0
        series = series * square + sign / math.factorial(power)
    return rest * series


def silu(value):
    return value / (1.0 + jnp.exp(-value))


def high_low(value):
    high = value.astype(jnp.bfloat16)
    return high, (value - high.astype(jnp.float32)).astype(jnp.bfloat16)


def front_kernel(
    part_index,
    parts,
    timestep,
    counts_far,
    tokens_far,
    positions_far,
    table_far,
    time_in_far,
    time_out_far,
    ada_weight_far,
    message,
    sums,
    x_in_ref,
    bias,
    row_valid,
    counts,
    tokens,
    positions,
    table,
    time_in,
    time_out,
    ada_weight,
    arrived,
):
    order = (
        (table_far, table),
        (time_in_far, time_in),
        (time_out_far, time_out),
        (ada_weight_far, ada_weight),
        (positions_far, positions),
        (tokens_far, tokens),
        (counts_far, counts),
    )
    copies = [
        pltpu.make_async_copy(far, near, arrived.at[index])
        for index, (far, near) in enumerate(order)
    ]
    for copy in copies:
        copy.start()
    rows, width = tokens.shape
    freq_size = time_in.shape[0]
    copies[0].wait()
    angle = timestep[0].astype(jnp.float32) * jnp.broadcast_to(
        table[3:4, :freq_size], (SUM_ROWS, freq_size)
    )
    shifted = jnp.broadcast_to(table[4:5, :freq_size], (SUM_ROWS, freq_size))
    features = sine(angle, shifted).astype(jnp.bfloat16)
    copies[1].wait()
    hidden = silu(jnp.dot(features, time_in[...], preferred_element_type=jnp.float32))
    copies[2].wait()
    cond = lax.dot_general(
        hidden.astype(jnp.bfloat16),
        time_out[...],
        (((1,), (1,)), ((), ())),
        preferred_element_type=jnp.float32,
    )
    copies[3].wait()
    partial = jnp.dot(
        silu(cond).astype(jnp.bfloat16), ada_weight[...], preferred_element_type=jnp.float32
    )
    sums[...] = pack_sums([partial[:, piece * width : (piece + 1) * width] for piece in range(3)])

    copies[4].wait()
    place = positions[...].astype(jnp.float32)
    same = lax.broadcasted_iota(jnp.int32, (rows, rows), 0) == lax.broadcasted_iota(
        jnp.int32, (rows, rows), 1
    )
    column = [
        jnp.sum(jnp.where(same, place[axis : axis + 1, :], 0.0), axis=1, keepdims=True)
        for axis in range(2)
    ]
    where_to = jnp.where(table[2:3, :] > 0.5, column[1], column[0])
    embed = sine(where_to * table[0:1, :], table[1:2, :])
    copies[5].wait()
    x_in = tokens[...].astype(jnp.float32) + embed
    x_in_ref[...] = x_in
    centered = x_in - jnp.mean(x_in, axis=1, keepdims=True)
    variance = jnp.mean(centered * centered, axis=1, keepdims=True)
    message[...] = (centered * lax.rsqrt(variance + 1e-06)).astype(jnp.bfloat16)

    copies[6].wait()
    my_index = lax.axis_index("patch")
    key_id = lax.broadcasted_iota(jnp.int32, bias.shape, 1)
    valid = key_id < 0
    for block in range(parts):
        first = block * rows
        used = counts[part_index(my_index, block)]
        valid = jnp.logical_or(valid, jnp.logical_and(key_id >= first, key_id < first + used))
    bias[...] = jnp.where(valid, 0.0, neg_large)
    own_row = lax.broadcasted_iota(jnp.int32, row_valid.shape, 0)
    row_valid[...] = (own_row < counts[my_index]).astype(jnp.float32)


def pack_sums(pieces):
    row_id = lax.broadcasted_iota(jnp.int32, pieces[0].shape, 0)
    packed = jnp.zeros(pieces[0].shape, jnp.float32)
    for piece, value in enumerate(pieces):
        high, low = high_low(value)
        packed = jnp.where(row_id == 2 * piece, high.astype(jnp.float32), packed)
        packed = jnp.where(row_id == 2 * piece + 1, low.astype(jnp.float32), packed)
    return packed.astype(jnp.bfloat16)


def sum_piece(value, piece):
    return value[2 * piece : 2 * piece + 1, :] + value[2 * piece + 1 : 2 * piece + 2, :]


def add_kernel(*refs):
    out = refs[-1]
    total = sum(ref[...].astype(jnp.float32) for ref in refs[:-1])
    out[...] = pack_sums(
        [jnp.broadcast_to(sum_piece(total, piece), out.shape) for piece in range(3)]
    )


def attend_rows(query_ref, start, rows, key_bias, keys, values, out):
    width = keys.shape[1]
    head_size = width // HEADS
    base_two = math.log2(math.e) / math.sqrt(head_size)
    lse_lane = lax.broadcasted_iota(jnp.int32, (rows, LANES), 1)
    lse_all = jnp.zeros((rows, LANES), jnp.float32)
    held = None
    tiles = []
    for group in head_groups(width):
        low, high = group[0] * head_size, (group[-1] + 1) * head_size
        first, last = low // LANES * LANES, -(-high // LANES) * LANES
        lane = lax.broadcasted_iota(jnp.int32, (1, last - first), 1) + first
        window = query_ref[start : start + rows, first:last]
        stacked = jnp.concatenate(
            [
                jnp.where(
                    jnp.logical_and(lane >= head * head_size, lane < (head + 1) * head_size),
                    window,
                    jnp.zeros((), jnp.bfloat16),
                )
                for head in group
            ],
            axis=0,
        )
        scores = lax.dot_general(
            stacked,
            keys[:, first:last],
            (((1,), (1,)), ((), ())),
            preferred_element_type=jnp.float32,
        )
        scores = scores + key_bias
        top = jnp.max(scores, axis=1, keepdims=True)
        weights = jnp.exp2((scores - top) * base_two)
        total = jnp.sum(weights, axis=1, keepdims=True)
        result = jnp.dot(
            weights.astype(jnp.bfloat16), values[:, first:last], preferred_element_type=jnp.float32
        )
        result = result * (1.0 / total)
        lse = top * base_two + jnp.log2(total)
        joined = result[:rows, :]
        for place, head in enumerate(group):
            mine = slice(place * rows, (place + 1) * rows)
            lse_all = jnp.where(lse_lane == head, lse[mine, :], lse_all)
            if place:
                joined = jnp.where(lane >= head * head_size, result[mine, :], joined)
        for begin in range(first, last, LANES):
            tile = joined[:, begin - first : begin - first + LANES]
            if begin < low:
                tile = jnp.where(lane[:, begin - first : begin - first + LANES] >= low, tile, held)
            if begin + LANES <= high:
                tiles.append(tile.astype(jnp.bfloat16))
            else:
                held = tile
    tiles.append(pack_lse(lse_all))
    for index, tile in enumerate(tiles):
        out[:, index * LANES : (index + 1) * LANES] = tile


def head_groups(width):
    head_size = width // HEADS
    groups = []
    head = 0
    while head < HEADS:
        first = head * head_size // LANES * LANES
        stop = head + 1
        while stop < HEADS and (stop + 1) * head_size <= first + 2 * LANES:
            stop += 1
        groups.append(tuple(range(head, stop)))
        head = stop
    return groups


def attend_kernel(block_rows, key_count, *refs):
    bias, sums_a, sums_b = refs[:3]
    key_refs = refs[3 : 3 + key_count]
    own, across, weight = refs[3 + key_count : 6 + key_count]
    own_query, keys, values, across_out = refs[6 + key_count : 10 + key_count]
    mod_keys, mod_queries, across_query = refs[10 + key_count :]
    width = weight.shape[0]
    sums = sums_a[...].astype(jnp.float32) + sums_b[...].astype(jnp.float32)
    shift = sum_piece(sums, 0)
    scale = 1.0 + sum_piece(sums, 1)

    def modulate(value):
        return (value.astype(jnp.float32) * scale + shift).astype(jnp.bfloat16)

    place = 0
    for ref in key_refs:
        for start in range(0, ref.shape[0], block_rows):
            mod_keys[place : place + block_rows, :] = modulate(ref[start : start + block_rows, :])
            place += block_rows
    mod_queries[:block_rows, :] = modulate(own[...])
    mod_queries[block_rows:, :] = modulate(across[...])
    piece = 3 * LANES
    for start in range(0, width, piece):
        stop = min(start + piece, width)
        both = jnp.dot(
            mod_queries[...], weight[:, start:stop], preferred_element_type=jnp.float32
        ).astype(jnp.bfloat16)
        own_query[:, start:stop] = both[:block_rows, :]
        across_query[:, start:stop] = both[block_rows:, :]
        keys[:, start:stop] = jnp.dot(
            mod_keys[...], weight[:, width + start : width + stop], preferred_element_type=jnp.float32
        ).astype(jnp.bfloat16)
        values[:, start:stop] = jnp.dot(
            mod_keys[...],
            weight[:, 2 * width + start : 2 * width + stop],
            preferred_element_type=jnp.float32,
        ).astype(jnp.bfloat16)
    attend_rows(across_query, 0, block_rows, bias[0:1, :], keys, values, across_out)


def own_kernel(bias, query, keys, values, out):
    attend_rows(query, 0, query.shape[0], bias[0:1, :], keys, values, out)


def pack_lse(lse):
    high = lse.astype(jnp.bfloat16).astype(jnp.float32)
    middle = (lse - high).astype(jnp.bfloat16).astype(jnp.float32)
    low = lse - high - middle
    return (high + pltpu.roll(middle, HEADS, 1) + pltpu.roll(low, 2 * HEADS, 1)).astype(
        jnp.bfloat16
    )


def unpack_lse(packed):
    source = lax.broadcasted_iota(jnp.int32, (LANES, LANES), 0)
    target = lax.broadcasted_iota(jnp.int32, (LANES, LANES), 1)
    chosen = source == target
    for piece in range(1, 3):
        chosen = jnp.logical_or(chosen, source == target + piece * HEADS)
    chosen = jnp.logical_and(chosen, target < HEADS).astype(jnp.bfloat16)
    return jnp.dot(packed, chosen, preferred_element_type=jnp.float32)


def spread(value, width):
    head_size = width // HEADS
    head_id = lax.broadcasted_iota(jnp.int32, (LANES, width), 0)
    lane_id = lax.broadcasted_iota(jnp.int32, (LANES, width), 1)
    low = head_id * head_size
    expand = jnp.logical_and(lane_id >= low, lane_id < low + head_size).astype(jnp.bfloat16)
    high, rest = high_low(value)
    return jnp.dot(high, expand, preferred_element_type=jnp.float32) + jnp.dot(
        rest, expand, preferred_element_type=jnp.float32
    )


def merge(packed_a, packed_b):
    width = packed_a.shape[1] - LANES
    lse_a, lse_b = unpack_lse(packed_a[:, width:]), unpack_lse(packed_b[:, width:])
    top = jnp.maximum(lse_a, lse_b)
    part_a = jnp.exp2(lse_a - top)
    part_b = jnp.exp2(lse_b - top)
    total = part_a + part_b
    share = spread(part_b / total, width)
    first = packed_a[:, :width].astype(jnp.float32)
    value = first + share * (packed_b[:, :width].astype(jnp.float32) - first)
    return value


def finish_kernel(packed_a, packed_b, x_in, row_valid, sums_a, sums_b, weight, out):
    value = merge(packed_a[...], packed_b[...])
    gate = sum_piece(sums_a[...].astype(jnp.float32) + sums_b[...].astype(jnp.float32), 2)
    projected = jnp.dot(
        value.astype(jnp.bfloat16), weight[...], preferred_element_type=jnp.float32
    )
    out[...] = (x_in[...] + gate * projected * row_valid[:, 0:1]).astype(jnp.bfloat16)


def far():
    return pl.BlockSpec(memory_space=pltpu.HBM)


def stay_far(array):
    return pltpu.with_memory_space_constraint(array, pltpu.HBM)


def per_device(
    tokens, positions, counts, timestep, time_in, time_out, ada_weight, qkv_weight, out_weight
):
    devices = lax.axis_size("patch")
    rows, width = tokens.shape
    shape = jax.ShapeDtypeStruct
    table = jnp.asarray(lane_table(width, time_in.shape[0]))
    far_masks = [mask for mask in range(devices) if not mask & (CORE_MASK | MERGE_MASK)]
    key_masks = far_masks + [mask | CORE_MASK for mask in far_masks]
    direct = devices <= DIRECT_LIMIT

    def swap(value, mask):
        pairs = [(index, index ^ mask) for index in range(devices)]
        return lax.ppermute(value, "patch", pairs)

    def part_index(my_index, block):
        if direct:
            return jnp.bitwise_xor(my_index, key_masks[block])
        return jnp.bitwise_and(my_index, MERGE_MASK) + sorted(key_masks)[block]

    inputs = (timestep, counts, tokens, positions, table, time_in, time_out.T, ada_weight)
    message, sums, x_in, bias, row_valid = pl.pallas_call(
        functools.partial(front_kernel, part_index, len(key_masks)),
        out_shape=(
            shape((rows, width), jnp.bfloat16),
            shape((SUM_ROWS, width), jnp.bfloat16),
            shape((rows, width), jnp.float32),
            shape((SUM_ROWS, rows * len(key_masks)), jnp.float32),
            shape((rows, LANES), jnp.float32),
        ),
        in_specs=[pl.BlockSpec(memory_space=pltpu.SMEM)] + [far()] * (len(inputs) - 1),
        out_specs=(vmem(),) * 5,
        scratch_shapes=[
            (pltpu.SMEM if array.ndim == 1 else pltpu.VMEM)(array.shape, array.dtype)
            for array in inputs[1:]
        ]
        + [pltpu.SemaphoreType.DMA((len(inputs) - 1,))],
        compiler_params=grant(8),
        name="front",
    )(inputs[0], *[stay_far(array) for array in inputs[1:]])

    def add(*addends):
        return pl.pallas_call(
            add_kernel,
            out_shape=shape((SUM_ROWS, width), jnp.bfloat16),
            in_specs=[vmem()] * len(addends),
            out_specs=vmem(),
            compiler_params=grant(4),
            cost_estimate=pl.CostEstimate(
                flops=1 << 34, bytes_accessed=4 * qkv_weight.size, transcendentals=0
            ),
            name="add",
        )(*addends)

    across = swap(message, MERGE_MASK)
    if direct:
        near = [message] + [swap(message, mask) for mask in far_masks[1:]]
        key_parts = near + [swap(part, CORE_MASK) for part in near]
        running = add(sums, swap(sums, CORE_MASK))
        running = add(running, *[swap(running, mask) for mask in far_masks[1:]])
        half_sums = running
        other_sums = swap(running, MERGE_MASK)
    else:
        groups = [[mask | rest for mask in sorted(key_masks)] for rest in (0, MERGE_MASK)]
        key_parts = [lax.all_gather(message, "patch", axis_index_groups=groups, tiled=True)]
        running = sums
        step = 1
        while 2 * step < devices:
            running = add(running, swap(running, step))
            step *= 2
        half_sums = running
        other_sums = swap(running, step)

    total_keys = rows * len(key_masks)
    own_query, keys, values, send = pl.pallas_call(
        functools.partial(attend_kernel, rows, len(key_parts)),
        out_shape=(
            shape((rows, width), jnp.bfloat16),
            shape((total_keys, width), jnp.bfloat16),
            shape((total_keys, width), jnp.bfloat16),
            shape((rows, width + LANES), jnp.bfloat16),
        ),
        in_specs=[vmem()] * (6 + len(key_parts)),
        out_specs=(vmem(),) * 4,
        scratch_shapes=[
            pltpu.VMEM((total_keys, width), jnp.bfloat16),
            pltpu.VMEM((2 * rows, width), jnp.bfloat16),
            pltpu.VMEM((rows, width), jnp.bfloat16),
        ],
        compiler_params=grant(ATTEND_GRANT if direct else 56),
        name="attend",
    )(bias, half_sums, other_sums, *key_parts, message, across, qkv_weight)
    own = pl.pallas_call(
        own_kernel,
        out_shape=shape((rows, width + LANES), jnp.bfloat16),
        in_specs=[vmem()] * 4,
        out_specs=vmem(),
        compiler_params=grant(8 if direct else 40),
        cost_estimate=pl.CostEstimate(
            flops=1 << 34, bytes_accessed=4 * keys.size, transcendentals=0
        ),
        name="own",
    )(bias, own_query, keys, values)
    return pl.pallas_call(
        finish_kernel,
        out_shape=shape((rows, width), jnp.bfloat16),
        in_specs=[vmem()] * 7,
        out_specs=vmem(),
        compiler_params=grant(8),
        name="finish",
    )(own, swap(send, MERGE_MASK), x_in, row_valid, half_sums, other_sums, out_weight)


def solution(mesh):
    placed = (
        P(("req", "patch"), None),
        P(None, ("req", "patch")),
        P("req"),
        P("req"),
        P(),
        P(None, "patch"),
        P("patch", None),
        P(),
        P(),
    )

    return jax.shard_map(
        per_device, mesh=mesh, in_specs=placed, out_specs=P(("req", "patch"), None), check_vma=False
    )
```

```python
import functools
import math

import jax
import jax.numpy as jnp
import numpy as np
from jax import lax
from jax.experimental import pallas as pl
from jax.experimental.pallas import tpu as pltpu
from jax.sharding import PartitionSpec as P


HEADS = 16
LANES = 128
SUM_ROWS = 8
CORE_MASK = 1
MERGE_MASK = 2
DIRECT_LIMIT = 16
ATTEND_GRANT = 24
neg_large = -1e30


def grant(mebibytes):
    return pltpu.CompilerParams(vmem_limit_bytes=mebibytes << 20)


def vmem():
    return pl.BlockSpec(memory_space=pltpu.VMEM)


def lane_table(model_width, freq_size):
    quarter = model_width // 4
    half = freq_size // 2
    lane = np.arange(model_width)
    table = np.zeros((SUM_ROWS, model_width), np.float32)
    table[0] = np.power(10000.0, -(lane % quarter) / quarter)
    table[1] = (lane // quarter) % 2
    table[2] = lane // (2 * quarter)
    feature = np.arange(freq_size)
    table[3, :freq_size] = np.exp(-math.log(10000.0) * (feature % half) / half)
    table[4, :freq_size] = feature < half
    return table


def sine(angle, shifted):
    turns = jnp.floor(angle * (0.5 / math.pi) + 0.5)
    rest = angle - turns * 6.28125
    rest = rest - turns * (2.0 * math.pi - 6.28125)
    rest = rest + shifted * (0.5 * math.pi)
    rest = jnp.where(rest > 0.5 * math.pi, math.pi - rest, rest)
    rest = jnp.where(rest < -0.5 * math.pi, -math.pi - rest, rest)
    square = rest * rest
    series = 1.0 / math.factorial(13)
    for power in (11, 9, 7, 5, 3, 1):
        sign = -1.0 if power % 4 == 3 else 1.0
        series = series * square + sign / math.factorial(power)
    return rest * series


def silu(value):
    return value / (1.0 + jnp.exp(-value))


def high_low(value):
    high = value.astype(jnp.bfloat16)
    return high, (value - high.astype(jnp.float32)).astype(jnp.bfloat16)


def front_kernel(
    part_index,
    parts,
    timestep,
    counts_far,
    tokens_far,
    positions_far,
    table_far,
    time_in_far,
    time_out_far,
    ada_weight_far,
    message,
    sums,
    x_in_ref,
    bias,
    row_valid,
    counts,
    tokens,
    positions,
    table,
    time_in,
    time_out,
    ada_weight,
    arrived,
):
    order = (
        (table_far, table),
        (positions_far, positions),
        (time_in_far, time_in),
        (time_out_far, time_out),
        (ada_weight_far, ada_weight),
        (tokens_far, tokens),
        (counts_far, counts),
    )
    copies = [
        pltpu.make_async_copy(far, near, arrived.at[index])
        for index, (far, near) in enumerate(order)
    ]
    for copy in copies:
        copy.start()
    rows, width = tokens.shape
    freq_size = time_in.shape[0]
    for copy in copies[:2]:
        copy.wait()
    place = positions[...].astype(jnp.float32)
    same = lax.broadcasted_iota(jnp.int32, (rows, rows), 0) == lax.broadcasted_iota(
        jnp.int32, (rows, rows), 1
    )
    column = [
        jnp.sum(jnp.where(same, place[axis : axis + 1, :], 0.0), axis=1, keepdims=True)
        for axis in range(2)
    ]
    where_to = jnp.where(table[2:3, :] > 0.5, column[1], column[0])
    embed = sine(where_to * table[0:1, :], table[1:2, :])
    angle = timestep[0].astype(jnp.float32) * jnp.broadcast_to(
        table[3:4, :freq_size], (SUM_ROWS, freq_size)
    )
    shifted = jnp.broadcast_to(table[4:5, :freq_size], (SUM_ROWS, freq_size))
    features = sine(angle, shifted).astype(jnp.bfloat16)
    for copy in copies[2:]:
        copy.wait()
    hidden = silu(jnp.dot(features, time_in[...], preferred_element_type=jnp.float32))
    cond = lax.dot_general(
        hidden.astype(jnp.bfloat16),
        time_out[...],
        (((1,), (1,)), ((), ())),
        preferred_element_type=jnp.float32,
    )
    partial = jnp.dot(
        silu(cond).astype(jnp.bfloat16), ada_weight[...], preferred_element_type=jnp.float32
    )
    x_in = tokens[...].astype(jnp.float32) + embed
    centered = x_in - jnp.mean(x_in, axis=1, keepdims=True)
    variance = jnp.mean(centered * centered, axis=1, keepdims=True)
    message[...] = (centered * lax.rsqrt(variance + 1e-06)).astype(jnp.bfloat16)
    x_in_ref[...] = x_in
    sums[...] = pack_sums([partial[:, piece * width : (piece + 1) * width] for piece in range(3)])

    my_index = lax.axis_index("patch")
    key_id = lax.broadcasted_iota(jnp.int32, bias.shape, 1)
    valid = key_id < 0
    for block in range(parts):
        first = block * rows
        used = counts[part_index(my_index, block)]
        valid = jnp.logical_or(valid, jnp.logical_and(key_id >= first, key_id < first + used))
    bias[...] = jnp.where(valid, 0.0, neg_large)
    own_row = lax.broadcasted_iota(jnp.int32, row_valid.shape, 0)
    row_valid[...] = (own_row < counts[my_index]).astype(jnp.float32)


def pack_sums(pieces):
    row_id = lax.broadcasted_iota(jnp.int32, pieces[0].shape, 0)
    packed = jnp.zeros(pieces[0].shape, jnp.float32)
    for piece, value in enumerate(pieces):
        high, low = high_low(value)
        packed = jnp.where(row_id == 2 * piece, high.astype(jnp.float32), packed)
        packed = jnp.where(row_id == 2 * piece + 1, low.astype(jnp.float32), packed)
    return packed.astype(jnp.bfloat16)


def sum_piece(value, piece):
    return value[2 * piece : 2 * piece + 1, :] + value[2 * piece + 1 : 2 * piece + 2, :]


def add_kernel(*refs):
    out = refs[-1]
    total = sum(ref[...].astype(jnp.float32) for ref in refs[:-1])
    out[...] = pack_sums(
        [jnp.broadcast_to(sum_piece(total, piece), out.shape) for piece in range(3)]
    )


def attend_rows(query_ref, rows, key_bias, keys, values, out):
    width = keys.shape[1]
    head_size = width // HEADS
    base_two = math.log2(math.e) / math.sqrt(head_size)
    lse_lane = lax.broadcasted_iota(jnp.int32, (rows, LANES), 1)
    lse_all = jnp.zeros((rows, LANES), jnp.float32)
    windows = [(first, min(first + 2 * LANES, width)) for first in range(0, width, 2 * LANES)]
    inside = [
        [
            head
            for head in range(HEADS)
            if head * head_size < last and (head + 1) * head_size > first
        ]
        for first, last in windows
    ]
    scores, weights, inverse, tiles = {}, {}, {}, []

    def lanes_of(head, first, last):
        lane = lax.broadcasted_iota(jnp.int32, (1, last - first), 1) + first
        return jnp.logical_and(lane >= head * head_size, lane < (head + 1) * head_size)

    def score(index):
        first, last = windows[index]
        window = query_ref[:, first:last]
        stacked = jnp.concatenate(
            [
                jnp.where(lanes_of(head, first, last), window, jnp.zeros((), jnp.bfloat16))
                for head in inside[index]
            ],
            axis=0,
        )
        result = lax.dot_general(
            stacked,
            keys[:, first:last],
            (((1,), (1,)), ((), ())),
            preferred_element_type=jnp.float32,
        )
        for place, head in enumerate(inside[index]):
            part = result[place * rows : (place + 1) * rows, :]
            scores[head] = scores[head] + part if head in scores else part

    score(0)
    for index, (first, last) in enumerate(windows):
        if index + 1 < len(windows):
            score(index + 1)
        for head in inside[index]:
            if head in weights:
                continue
            value = scores.pop(head) + key_bias
            top = jnp.max(value, axis=1, keepdims=True)
            value = jnp.exp2((value - top) * base_two)
            total = jnp.sum(value, axis=1, keepdims=True)
            weights[head] = value.astype(jnp.bfloat16)
            inverse[head] = 1.0 / total
            lse_all = jnp.where(lse_lane == head, top * base_two + jnp.log2(total), lse_all)
        result = jnp.dot(
            jnp.concatenate([weights[head] for head in inside[index]], axis=0),
            values[:, first:last],
            preferred_element_type=jnp.float32,
        )
        joined = None
        for place, head in enumerate(inside[index]):
            part = result[place * rows : (place + 1) * rows, :] * inverse[head]
            if joined is None:
                joined = part
            else:
                joined = jnp.where(lanes_of(head, first, last), part, joined)
        tiles.append((first, last, joined.astype(jnp.bfloat16)))
    for first, last, tile in tiles:
        out[:, first:last] = tile
    out[:, width:] = pack_lse(lse_all)


def attend_kernel(block_rows, key_count, *refs):
    bias, sums_a, sums_b = refs[:3]
    key_refs = refs[3 : 3 + key_count]
    own, across, weight = refs[3 + key_count : 6 + key_count]
    own_query, keys, values, across_out = refs[6 + key_count : 10 + key_count]
    mod_keys, mod_queries, across_query = refs[10 + key_count :]
    width = weight.shape[0]
    sums = sums_a[...].astype(jnp.float32) + sums_b[...].astype(jnp.float32)
    shift = sum_piece(sums, 0)
    scale = 1.0 + sum_piece(sums, 1)

    def modulate(value):
        return (value.astype(jnp.float32) * scale + shift).astype(jnp.bfloat16)

    place = 0
    for ref in key_refs:
        for start in range(0, ref.shape[0], block_rows):
            mod_keys[place : place + block_rows, :] = modulate(ref[start : start + block_rows, :])
            place += block_rows
    mod_queries[:block_rows, :] = modulate(own[...])
    mod_queries[block_rows:, :] = modulate(across[...])
    piece = 3 * LANES
    for start in range(0, width, piece):
        stop = min(start + piece, width)
        both = jnp.dot(
            mod_queries[...], weight[:, start:stop], preferred_element_type=jnp.float32
        ).astype(jnp.bfloat16)
        own_query[:, start:stop] = both[:block_rows, :]
        across_query[:, start:stop] = both[block_rows:, :]
        keys[:, start:stop] = jnp.dot(
            mod_keys[...], weight[:, width + start : width + stop], preferred_element_type=jnp.float32
        ).astype(jnp.bfloat16)
        values[:, start:stop] = jnp.dot(
            mod_keys[...],
            weight[:, 2 * width + start : 2 * width + stop],
            preferred_element_type=jnp.float32,
        ).astype(jnp.bfloat16)
    attend_rows(across_query, block_rows, bias[0:1, :], keys, values, across_out)


def own_kernel(bias, query, keys, values, out):
    attend_rows(query, query.shape[0], bias[0:1, :], keys, values, out)


def pack_lse(lse):
    high = lse.astype(jnp.bfloat16).astype(jnp.float32)
    middle = (lse - high).astype(jnp.bfloat16).astype(jnp.float32)
    low = lse - high - middle
    return (high + pltpu.roll(middle, HEADS, 1) + pltpu.roll(low, 2 * HEADS, 1)).astype(
        jnp.bfloat16
    )


def unpack_lse(packed):
    source = lax.broadcasted_iota(jnp.int32, (LANES, LANES), 0)
    target = lax.broadcasted_iota(jnp.int32, (LANES, LANES), 1)
    chosen = source == target
    for piece in range(1, 3):
        chosen = jnp.logical_or(chosen, source == target + piece * HEADS)
    chosen = jnp.logical_and(chosen, target < HEADS).astype(jnp.bfloat16)
    return jnp.dot(packed, chosen, preferred_element_type=jnp.float32)


def spread(value, width):
    head_size = width // HEADS
    head_id = lax.broadcasted_iota(jnp.int32, (LANES, width), 0)
    lane_id = lax.broadcasted_iota(jnp.int32, (LANES, width), 1)
    low = head_id * head_size
    expand = jnp.logical_and(lane_id >= low, lane_id < low + head_size).astype(jnp.bfloat16)
    high, rest = high_low(value)
    return jnp.dot(high, expand, preferred_element_type=jnp.float32) + jnp.dot(
        rest, expand, preferred_element_type=jnp.float32
    )


def merge(packed_a, packed_b):
    width = packed_a.shape[1] - LANES
    lse_a, lse_b = unpack_lse(packed_a[:, width:]), unpack_lse(packed_b[:, width:])
    top = jnp.maximum(lse_a, lse_b)
    part_a = jnp.exp2(lse_a - top)
    part_b = jnp.exp2(lse_b - top)
    total = part_a + part_b
    share = spread(part_b / total, width)
    first = packed_a[:, :width].astype(jnp.float32)
    value = first + share * (packed_b[:, :width].astype(jnp.float32) - first)
    return value


def finish_kernel(packed_a, packed_b, x_in, row_valid, sums_a, sums_b, weight, out):
    value = merge(packed_a[...], packed_b[...])
    gate = sum_piece(sums_a[...].astype(jnp.float32) + sums_b[...].astype(jnp.float32), 2)
    projected = jnp.dot(
        value.astype(jnp.bfloat16), weight[...], preferred_element_type=jnp.float32
    )
    out[...] = (x_in[...] + gate * projected * row_valid[:, 0:1]).astype(jnp.bfloat16)


def far():
    return pl.BlockSpec(memory_space=pltpu.HBM)


def stay_far(array):
    return pltpu.with_memory_space_constraint(array, pltpu.HBM)


def per_device(
    tokens, positions, counts, timestep, time_in, time_out, ada_weight, qkv_weight, out_weight
):
    devices = lax.axis_size("patch")
    rows, width = tokens.shape
    shape = jax.ShapeDtypeStruct
    table = jnp.asarray(lane_table(width, time_in.shape[0]))
    far_masks = [mask for mask in range(devices) if not mask & (CORE_MASK | MERGE_MASK)]
    key_masks = far_masks + [mask | CORE_MASK for mask in far_masks]
    direct = devices <= DIRECT_LIMIT

    def swap(value, mask):
        pairs = [(index, index ^ mask) for index in range(devices)]
        return lax.ppermute(value, "patch", pairs)

    def part_index(my_index, block):
        if direct:
            return jnp.bitwise_xor(my_index, key_masks[block])
        return jnp.bitwise_and(my_index, MERGE_MASK) + sorted(key_masks)[block]

    inputs = (timestep, counts, tokens, positions, table, time_in, time_out.T, ada_weight)
    message, sums, x_in, bias, row_valid = pl.pallas_call(
        functools.partial(front_kernel, part_index, len(key_masks)),
        out_shape=(
            shape((rows, width), jnp.bfloat16),
            shape((SUM_ROWS, width), jnp.bfloat16),
            shape((rows, width), jnp.float32),
            shape((SUM_ROWS, rows * len(key_masks)), jnp.float32),
            shape((rows, LANES), jnp.float32),
        ),
        in_specs=[pl.BlockSpec(memory_space=pltpu.SMEM)] + [far()] * (len(inputs) - 1),
        out_specs=(vmem(),) * 5,
        scratch_shapes=[
            (pltpu.SMEM if array.ndim == 1 else pltpu.VMEM)(array.shape, array.dtype)
            for array in inputs[1:]
        ]
        + [pltpu.SemaphoreType.DMA((len(inputs) - 1,))],
        compiler_params=grant(8),
        name="front",
    )(inputs[0], *[stay_far(array) for array in inputs[1:]])

    def add(*addends):
        return pl.pallas_call(
            add_kernel,
            out_shape=shape((SUM_ROWS, width), jnp.bfloat16),
            in_specs=[vmem()] * len(addends),
            out_specs=vmem(),
            compiler_params=grant(4),
            cost_estimate=pl.CostEstimate(
                flops=1 << 34, bytes_accessed=4 * qkv_weight.size, transcendentals=0
            ),
            name="add",
        )(*addends)

    across = swap(message, MERGE_MASK)
    if direct:
        near = [message] + [swap(message, mask) for mask in far_masks[1:]]
        key_parts = near + [swap(part, CORE_MASK) for part in near]
        running = add(sums, swap(sums, CORE_MASK))
        running = add(running, *[swap(running, mask) for mask in far_masks[1:]])
        half_sums = running
        other_sums = swap(running, MERGE_MASK)
    else:
        groups = [[mask | rest for mask in sorted(key_masks)] for rest in (0, MERGE_MASK)]
        key_parts = [lax.all_gather(message, "patch", axis_index_groups=groups, tiled=True)]
        running = sums
        step = 1
        while 2 * step < devices:
            running = add(running, swap(running, step))
            step *= 2
        half_sums = running
        other_sums = swap(running, step)

    total_keys = rows * len(key_masks)
    own_query, keys, values, send = pl.pallas_call(
        functools.partial(attend_kernel, rows, len(key_parts)),
        out_shape=(
            shape((rows, width), jnp.bfloat16),
            shape((total_keys, width), jnp.bfloat16),
            shape((total_keys, width), jnp.bfloat16),
            shape((rows, width + LANES), jnp.bfloat16),
        ),
        in_specs=[vmem()] * (6 + len(key_parts)),
        out_specs=(vmem(),) * 4,
        scratch_shapes=[
            pltpu.VMEM((total_keys, width), jnp.bfloat16),
            pltpu.VMEM((2 * rows, width), jnp.bfloat16),
            pltpu.VMEM((rows, width), jnp.bfloat16),
        ],
        compiler_params=grant(ATTEND_GRANT if direct else 56),
        name="attend",
    )(bias, half_sums, other_sums, *key_parts, message, across, qkv_weight)
    own = pl.pallas_call(
        own_kernel,
        out_shape=shape((rows, width + LANES), jnp.bfloat16),
        in_specs=[vmem()] * 4,
        out_specs=vmem(),
        compiler_params=grant(8 if direct else 40),
        cost_estimate=pl.CostEstimate(
            flops=1 << 34, bytes_accessed=4 * keys.size, transcendentals=0
        ),
        name="own",
    )(bias, own_query, keys, values)
    return pl.pallas_call(
        finish_kernel,
        out_shape=shape((rows, width), jnp.bfloat16),
        in_specs=[vmem()] * 7,
        out_specs=vmem(),
        compiler_params=grant(8),
        name="finish",
    )(own, swap(send, MERGE_MASK), x_in, row_valid, half_sums, other_sums, out_weight)


def solution(mesh):
    placed = (
        P(("req", "patch"), None),
        P(None, ("req", "patch")),
        P("req"),
        P("req"),
        P(),
        P(None, "patch"),
        P("patch", None),
        P(),
        P(),
    )

    return jax.shard_map(
        per_device, mesh=mesh, in_specs=placed, out_specs=P(("req", "patch"), None), check_vma=False
    )
```

```python
import functools
import math

import jax
import jax.numpy as jnp
import numpy as np
from jax import lax
from jax.experimental import pallas as pl
from jax.experimental.pallas import tpu as pltpu
from jax.sharding import PartitionSpec as P


HEADS = 16
LANES = 128
PIECE = 768
SUM_ROWS = 8
CORE_MASK = 1
MERGE_MASK = 2
DIRECT_LIMIT = 16
ATTEND_GRANT = 24
neg_large = -1e30


def grant(mebibytes):
    return pltpu.CompilerParams(vmem_limit_bytes=mebibytes << 20)


def vmem():
    return pl.BlockSpec(memory_space=pltpu.VMEM)


def lane_table(model_width, freq_size):
    quarter = model_width // 4
    half = freq_size // 2
    lane = np.arange(model_width)
    table = np.zeros((SUM_ROWS, model_width), np.float32)
    table[0] = np.power(10000.0, -(lane % quarter) / quarter)
    table[1] = (lane // quarter) % 2
    table[2] = lane // (2 * quarter)
    feature = np.arange(freq_size)
    table[3, :freq_size] = np.exp(-math.log(10000.0) * (feature % half) / half)
    table[4, :freq_size] = feature < half
    return table


def sine(angle, shifted):
    turns = jnp.floor(angle * (0.5 / math.pi) + 0.5)
    rest = angle - turns * 6.28125
    rest = rest - turns * (2.0 * math.pi - 6.28125)
    rest = rest + shifted * (0.5 * math.pi)
    rest = jnp.where(rest > 0.5 * math.pi, math.pi - rest, rest)
    rest = jnp.where(rest < -0.5 * math.pi, -math.pi - rest, rest)
    square = rest * rest
    series = 1.0 / math.factorial(13)
    for power in (11, 9, 7, 5, 3, 1):
        sign = -1.0 if power % 4 == 3 else 1.0
        series = series * square + sign / math.factorial(power)
    return rest * series


def silu(value):
    return value / (1.0 + jnp.exp(-value))


def high_low(value):
    high = value.astype(jnp.bfloat16)
    return high, (value - high.astype(jnp.float32)).astype(jnp.bfloat16)


def front_kernel(
    part_index,
    parts,
    timestep,
    counts_far,
    tokens_far,
    positions_far,
    table_far,
    time_in_far,
    time_out_far,
    ada_weight_far,
    message,
    sums,
    x_in_ref,
    bias,
    row_valid,
    counts,
    tokens,
    positions,
    table,
    time_in,
    time_out,
    ada_weight,
    arrived,
):
    order = (
        (table_far, table),
        (positions_far, positions),
        (tokens_far, tokens),
        (time_in_far, time_in),
        (time_out_far, time_out),
        (ada_weight_far, ada_weight),
        (counts_far, counts),
    )
    copies = [
        pltpu.make_async_copy(far, near, arrived.at[index])
        for index, (far, near) in enumerate(order)
    ]
    for copy in copies:
        copy.start()
    rows, width = tokens.shape
    freq_size = time_in.shape[0]
    for copy in copies[:3]:
        copy.wait()
    place = positions[...].astype(jnp.float32)
    same = lax.broadcasted_iota(jnp.int32, (rows, rows), 0) == lax.broadcasted_iota(
        jnp.int32, (rows, rows), 1
    )
    column = [
        jnp.sum(jnp.where(same, place[axis : axis + 1, :], 0.0), axis=1, keepdims=True)
        for axis in range(2)
    ]
    for start in range(0, rows, SUM_ROWS):
        chunk = slice(start, start + SUM_ROWS)
        where_to = jnp.where(table[2:3, :] > 0.5, column[1][chunk, :], column[0][chunk, :])
        x_in_ref[chunk, :] = tokens[chunk, :].astype(jnp.float32) + sine(
            where_to * table[0:1, :], jnp.broadcast_to(table[1:2, :], where_to.shape)
        )
    angle = timestep[0].astype(jnp.float32) * jnp.broadcast_to(
        table[3:4, :freq_size], (SUM_ROWS, freq_size)
    )
    shifted = jnp.broadcast_to(table[4:5, :freq_size], (SUM_ROWS, freq_size))
    features = sine(angle, shifted).astype(jnp.bfloat16)
    for copy in copies[3:]:
        copy.wait()
    hidden = silu(jnp.dot(features, time_in[...], preferred_element_type=jnp.float32))
    cond = lax.dot_general(
        hidden.astype(jnp.bfloat16),
        time_out[...],
        (((1,), (1,)), ((), ())),
        preferred_element_type=jnp.float32,
    )
    partial = jnp.dot(
        silu(cond).astype(jnp.bfloat16), ada_weight[...], preferred_element_type=jnp.float32
    )
    x_in = x_in_ref[...]
    centered = x_in - jnp.mean(x_in, axis=1, keepdims=True)
    variance = jnp.mean(centered * centered, axis=1, keepdims=True)
    message[...] = (centered * lax.rsqrt(variance + 1e-06)).astype(jnp.bfloat16)
    sums[...] = pack_sums([partial[:, piece * width : (piece + 1) * width] for piece in range(3)])

    my_index = lax.axis_index("patch")
    key_id = lax.broadcasted_iota(jnp.int32, bias.shape, 1)
    valid = key_id < 0
    for block in range(parts):
        first = block * rows
        used = counts[part_index(my_index, block)]
        valid = jnp.logical_or(valid, jnp.logical_and(key_id >= first, key_id < first + used))
    bias[...] = jnp.where(valid, 0.0, neg_large)
    own_row = lax.broadcasted_iota(jnp.int32, row_valid.shape, 0)
    row_valid[...] = (own_row < counts[my_index]).astype(jnp.float32)


def pack_sums(pieces):
    row_id = lax.broadcasted_iota(jnp.int32, pieces[0].shape, 0)
    packed = jnp.zeros(pieces[0].shape, jnp.float32)
    for piece, value in enumerate(pieces):
        high, low = high_low(value)
        packed = jnp.where(row_id == 2 * piece, high.astype(jnp.float32), packed)
        packed = jnp.where(row_id == 2 * piece + 1, low.astype(jnp.float32), packed)
    return packed.astype(jnp.bfloat16)


def sum_piece(value, piece):
    return value[2 * piece : 2 * piece + 1, :] + value[2 * piece + 1 : 2 * piece + 2, :]


def add_kernel(*refs):
    out = refs[-1]
    total = sum(ref[...].astype(jnp.float32) for ref in refs[:-1])
    out[...] = pack_sums(
        [jnp.broadcast_to(sum_piece(total, piece), out.shape) for piece in range(3)]
    )


def attend_rows(query_ref, rows, key_bias, keys, values, out):
    width = keys.shape[1]
    head_size = width // HEADS
    base_two = math.log2(math.e) / math.sqrt(head_size)
    lse_lane = lax.broadcasted_iota(jnp.int32, (rows, LANES), 1)
    lse_all = jnp.zeros((rows, LANES), jnp.float32)
    windows = [(first, min(first + 2 * LANES, width)) for first in range(0, width, 2 * LANES)]
    inside = [
        [
            head
            for head in range(HEADS)
            if head * head_size < last and (head + 1) * head_size > first
        ]
        for first, last in windows
    ]
    scores, weights, inverse, tiles = {}, {}, {}, []

    def lanes_of(head, first, last):
        lane = lax.broadcasted_iota(jnp.int32, (1, last - first), 1) + first
        return jnp.logical_and(lane >= head * head_size, lane < (head + 1) * head_size)

    def score(index):
        first, last = windows[index]
        window = query_ref[:, first:last]
        stacked = jnp.concatenate(
            [
                jnp.where(lanes_of(head, first, last), window, jnp.zeros((), jnp.bfloat16))
                for head in inside[index]
            ],
            axis=0,
        )
        result = lax.dot_general(
            stacked,
            keys[:, first:last],
            (((1,), (1,)), ((), ())),
            preferred_element_type=jnp.float32,
        )
        for place, head in enumerate(inside[index]):
            part = result[place * rows : (place + 1) * rows, :]
            scores[head] = scores[head] + part if head in scores else part

    score(0)
    for index, (first, last) in enumerate(windows):
        if index + 1 < len(windows):
            score(index + 1)
        for head in inside[index]:
            if head in weights:
                continue
            value = scores.pop(head) + key_bias
            top = jnp.max(value, axis=1, keepdims=True)
            value = jnp.exp2((value - top) * base_two)
            total = jnp.sum(value, axis=1, keepdims=True)
            weights[head] = value.astype(jnp.bfloat16)
            inverse[head] = 1.0 / total
            lse_all = jnp.where(lse_lane == head, top * base_two + jnp.log2(total), lse_all)
        result = jnp.dot(
            jnp.concatenate([weights[head] for head in inside[index]], axis=0),
            values[:, first:last],
            preferred_element_type=jnp.float32,
        )
        joined = None
        for place, head in enumerate(inside[index]):
            part = result[place * rows : (place + 1) * rows, :] * inverse[head]
            if joined is None:
                joined = part
            else:
                joined = jnp.where(lanes_of(head, first, last), part, joined)
        tiles.append((first, last, joined.astype(jnp.bfloat16)))
    for first, last, tile in tiles:
        out[:, first:last] = tile
    out[:, width:] = pack_lse(lse_all)


def attend_kernel(block_rows, key_count, *refs):
    bias, sums_a, sums_b = refs[:3]
    key_refs = refs[3 : 3 + key_count]
    own, across, weight = refs[3 + key_count : 6 + key_count]
    own_query, keys, values, across_out = refs[6 + key_count : 10 + key_count]
    mod_keys, mod_queries, across_query = refs[10 + key_count :]
    width = weight.shape[0]
    sums = sums_a[...].astype(jnp.float32) + sums_b[...].astype(jnp.float32)
    shift = sum_piece(sums, 0)
    scale = 1.0 + sum_piece(sums, 1)

    def modulate(value):
        return (value.astype(jnp.float32) * scale + shift).astype(jnp.bfloat16)

    place = 0
    for ref in key_refs:
        for start in range(0, ref.shape[0], block_rows):
            mod_keys[place : place + block_rows, :] = modulate(ref[start : start + block_rows, :])
            place += block_rows
    mod_queries[:block_rows, :] = modulate(own[...])
    mod_queries[block_rows:, :] = modulate(across[...])
    for start in range(0, width, PIECE):
        stop = min(start + PIECE, width)
        both = jnp.dot(
            mod_queries[...], weight[:, start:stop], preferred_element_type=jnp.float32
        ).astype(jnp.bfloat16)
        own_query[:, start:stop] = both[:block_rows, :]
        across_query[:, start:stop] = both[block_rows:, :]
    for start in range(0, 2 * width, PIECE):
        stop = min(start + PIECE, 2 * width)
        both = jnp.dot(
            mod_keys[...], weight[:, width + start : width + stop], preferred_element_type=jnp.float32
        ).astype(jnp.bfloat16)
        split = min(max(width - start, 0), stop - start)
        if split:
            keys[:, start : start + split] = both[:, :split]
        if split < stop - start:
            values[:, start + split - width : stop - width] = both[:, split:]
    attend_rows(across_query, block_rows, bias[0:1, :], keys, values, across_out)


def own_kernel(bias, query, keys, values, out, lse, expand):
    width = query.shape[1]
    head_size = width // HEADS
    attend_rows(query, query.shape[0], bias[0:1, :], keys, values, out)
    lse[...] = unpack_lse(out[:, width:])
    head_id = lax.broadcasted_iota(jnp.int32, expand.shape, 0)
    lane_id = lax.broadcasted_iota(jnp.int32, expand.shape, 1)
    low = head_id * head_size
    inside = jnp.logical_and(lane_id >= low, lane_id < low + head_size)
    expand[...] = inside.astype(jnp.float32).astype(jnp.bfloat16)


def pack_lse(lse):
    high = lse.astype(jnp.bfloat16).astype(jnp.float32)
    middle = (lse - high).astype(jnp.bfloat16).astype(jnp.float32)
    low = lse - high - middle
    return (high + pltpu.roll(middle, HEADS, 1) + pltpu.roll(low, 2 * HEADS, 1)).astype(
        jnp.bfloat16
    )


def unpack_lse(packed):
    source = lax.broadcasted_iota(jnp.int32, (LANES, LANES), 0)
    target = lax.broadcasted_iota(jnp.int32, (LANES, LANES), 1)
    chosen = source == target
    for piece in range(1, 3):
        chosen = jnp.logical_or(chosen, source == target + piece * HEADS)
    chosen = jnp.logical_and(chosen, target < HEADS).astype(jnp.bfloat16)
    return jnp.dot(packed, chosen, preferred_element_type=jnp.float32)


def merge(value_a, lse_a, packed_b, expand):
    width = value_a.shape[1] - LANES
    lse_b = unpack_lse(packed_b[:, width:])
    top = jnp.maximum(lse_a, lse_b)
    part_a = jnp.exp2(lse_a - top)
    part_b = jnp.exp2(lse_b - top)
    high, rest = high_low(part_b / (part_a + part_b))
    share = jnp.dot(high, expand, preferred_element_type=jnp.float32) + jnp.dot(
        rest, expand, preferred_element_type=jnp.float32
    )
    first = value_a[:, :width].astype(jnp.float32)
    return first + share * (packed_b[:, :width].astype(jnp.float32) - first)


def finish_kernel(
    value_a, lse_a, expand, packed_b, x_in, row_valid, sums_a, sums_b, weight, out
):
    value = merge(value_a[...], lse_a[...], packed_b[...], expand[...])
    gate = sum_piece(sums_a[...].astype(jnp.float32) + sums_b[...].astype(jnp.float32), 2)
    projected = jnp.dot(
        value.astype(jnp.bfloat16), weight[...], preferred_element_type=jnp.float32
    )
    out[...] = (x_in[...] + gate * projected * row_valid[:, 0:1]).astype(jnp.bfloat16)


def far():
    return pl.BlockSpec(memory_space=pltpu.HBM)


def stay_far(array):
    return pltpu.with_memory_space_constraint(array, pltpu.HBM)


def per_device(
    tokens, positions, counts, timestep, time_in, time_out, ada_weight, qkv_weight, out_weight
):
    devices = lax.axis_size("patch")
    rows, width = tokens.shape
    shape = jax.ShapeDtypeStruct
    table = jnp.asarray(lane_table(width, time_in.shape[0]))
    far_masks = [mask for mask in range(devices) if not mask & (CORE_MASK | MERGE_MASK)]
    key_masks = far_masks + [mask | CORE_MASK for mask in far_masks]
    direct = devices <= DIRECT_LIMIT

    def swap(value, mask):
        pairs = [(index, index ^ mask) for index in range(devices)]
        return lax.ppermute(value, "patch", pairs)

    def part_index(my_index, block):
        if direct:
            return jnp.bitwise_xor(my_index, key_masks[block])
        return jnp.bitwise_and(my_index, MERGE_MASK) + sorted(key_masks)[block]

    inputs = (timestep, counts, tokens, positions, table, time_in, time_out.T, ada_weight)
    message, sums, x_in, bias, row_valid = pl.pallas_call(
        functools.partial(front_kernel, part_index, len(key_masks)),
        out_shape=(
            shape((rows, width), jnp.bfloat16),
            shape((SUM_ROWS, width), jnp.bfloat16),
            shape((rows, width), jnp.float32),
            shape((SUM_ROWS, rows * len(key_masks)), jnp.float32),
            shape((rows, LANES), jnp.float32),
        ),
        in_specs=[pl.BlockSpec(memory_space=pltpu.SMEM)] + [far()] * (len(inputs) - 1),
        out_specs=(vmem(),) * 5,
        scratch_shapes=[
            (pltpu.SMEM if array.ndim == 1 else pltpu.VMEM)(array.shape, array.dtype)
            for array in inputs[1:]
        ]
        + [pltpu.SemaphoreType.DMA((len(inputs) - 1,))],
        compiler_params=grant(8),
        name="front",
    )(inputs[0], *[stay_far(array) for array in inputs[1:]])

    def add(*addends):
        return pl.pallas_call(
            add_kernel,
            out_shape=shape((SUM_ROWS, width), jnp.bfloat16),
            in_specs=[vmem()] * len(addends),
            out_specs=vmem(),
            compiler_params=grant(4),
            cost_estimate=pl.CostEstimate(
                flops=1 << 34, bytes_accessed=4 * qkv_weight.size, transcendentals=0
            ),
            name="add",
        )(*addends)

    across = swap(message, MERGE_MASK)
    if direct:
        near = [message] + [swap(message, mask) for mask in far_masks[1:]]
        key_parts = near + [swap(part, CORE_MASK) for part in near]
        running = add(sums, swap(sums, CORE_MASK))
        running = add(running, *[swap(running, mask) for mask in far_masks[1:]])
        half_sums = running
        other_sums = swap(running, MERGE_MASK)
    else:
        groups = [[mask | rest for mask in sorted(key_masks)] for rest in (0, MERGE_MASK)]
        key_parts = [lax.all_gather(message, "patch", axis_index_groups=groups, tiled=True)]
        running = sums
        step = 1
        while 2 * step < devices:
            running = add(running, swap(running, step))
            step *= 2
        half_sums = running
        other_sums = swap(running, step)

    total_keys = rows * len(key_masks)
    own_query, keys, values, send = pl.pallas_call(
        functools.partial(attend_kernel, rows, len(key_parts)),
        out_shape=(
            shape((rows, width), jnp.bfloat16),
            shape((total_keys, width), jnp.bfloat16),
            shape((total_keys, width), jnp.bfloat16),
            shape((rows, width + LANES), jnp.bfloat16),
        ),
        in_specs=[vmem()] * (6 + len(key_parts)),
        out_specs=(vmem(),) * 4,
        scratch_shapes=[
            pltpu.VMEM((total_keys, width), jnp.bfloat16),
            pltpu.VMEM((2 * rows, width), jnp.bfloat16),
            pltpu.VMEM((rows, width), jnp.bfloat16),
        ],
        compiler_params=grant(ATTEND_GRANT if direct else 56),
        name="attend",
    )(bias, half_sums, other_sums, *key_parts, message, across, qkv_weight)
    own, own_lse, expand = pl.pallas_call(
        own_kernel,
        out_shape=(
            shape((rows, width + LANES), jnp.bfloat16),
            shape((rows, LANES), jnp.float32),
            shape((LANES, width), jnp.bfloat16),
        ),
        in_specs=[vmem()] * 4,
        out_specs=(vmem(),) * 3,
        compiler_params=grant(8 if direct else 40),
        cost_estimate=pl.CostEstimate(
            flops=1 << 34, bytes_accessed=4 * keys.size, transcendentals=0
        ),
        name="own",
    )(bias, own_query, keys, values)
    return pl.pallas_call(
        finish_kernel,
        out_shape=shape((rows, width), jnp.bfloat16),
        in_specs=[vmem()] * 9,
        out_specs=vmem(),
        compiler_params=grant(8),
        name="finish",
    )(
        own,
        own_lse,
        expand,
        swap(send, MERGE_MASK),
        x_in,
        row_valid,
        half_sums,
        other_sums,
        out_weight,
    )


def solution(mesh):
    placed = (
        P(("req", "patch"), None),
        P(None, ("req", "patch")),
        P("req"),
        P("req"),
        P(),
        P(None, "patch"),
        P("patch", None),
        P(),
        P(),
    )

    return jax.shard_map(
        per_device, mesh=mesh, in_specs=placed, out_specs=P(("req", "patch"), None), check_vma=False
    )
```

```python
import functools
import math

import jax
import jax.numpy as jnp
import numpy as np
from jax import lax
from jax.experimental import pallas as pl
from jax.experimental.pallas import tpu as pltpu
from jax.sharding import PartitionSpec as P


HEADS = 16
LANES = 128
PIECE = 768
FINISH_PIECE = 512
SUM_ROWS = 8
CORE_MASK = 1
MERGE_MASK = 2
DIRECT_LIMIT = 16
ATTEND_GRANT = 24
neg_large = -1e30


def grant(mebibytes):
    return pltpu.CompilerParams(vmem_limit_bytes=mebibytes << 20)


def vmem():
    return pl.BlockSpec(memory_space=pltpu.VMEM)


def lane_table(model_width, freq_size):
    quarter = model_width // 4
    half = freq_size // 2
    lane = np.arange(model_width)
    table = np.zeros((SUM_ROWS, model_width), np.float32)
    table[0] = np.power(10000.0, -(lane % quarter) / quarter)
    table[1] = (lane // quarter) % 2
    table[2] = lane // (2 * quarter)
    feature = np.arange(freq_size)
    table[3, :freq_size] = np.exp(-math.log(10000.0) * (feature % half) / half)
    table[4, :freq_size] = feature < half
    return table


def sine(angle, shifted):
    turns = jnp.floor(angle * (0.5 / math.pi) + 0.5)
    rest = angle - turns * 6.28125
    rest = rest - turns * (2.0 * math.pi - 6.28125)
    rest = rest + shifted * (0.5 * math.pi)
    rest = jnp.where(rest > 0.5 * math.pi, math.pi - rest, rest)
    rest = jnp.where(rest < -0.5 * math.pi, -math.pi - rest, rest)
    square = rest * rest
    series = 1.0 / math.factorial(13)
    for power in (11, 9, 7, 5, 3, 1):
        sign = -1.0 if power % 4 == 3 else 1.0
        series = series * square + sign / math.factorial(power)
    return rest * series


def silu(value):
    return value / (1.0 + jnp.exp(-value))


def high_low(value):
    high = value.astype(jnp.bfloat16)
    return high, (value - high.astype(jnp.float32)).astype(jnp.bfloat16)


def front_kernel(
    part_index,
    parts,
    timestep,
    counts_far,
    tokens_far,
    positions_far,
    table_far,
    time_in_far,
    time_out_far,
    ada_weight_far,
    message,
    sums,
    x_in_ref,
    bias,
    row_valid,
    counts,
    tokens,
    positions,
    table,
    time_in,
    time_out,
    ada_weight,
    arrived,
):
    order = (
        (table_far, table),
        (positions_far, positions),
        (tokens_far, tokens),
        (time_in_far, time_in),
        (time_out_far, time_out),
        (ada_weight_far, ada_weight),
        (counts_far, counts),
    )
    copies = [
        pltpu.make_async_copy(far, near, arrived.at[index])
        for index, (far, near) in enumerate(order)
    ]
    for copy in copies:
        copy.start()
    rows, width = tokens.shape
    freq_size = time_in.shape[0]
    for copy in copies[:3]:
        copy.wait()
    place = positions[...].astype(jnp.float32)
    same = lax.broadcasted_iota(jnp.int32, (rows, rows), 0) == lax.broadcasted_iota(
        jnp.int32, (rows, rows), 1
    )
    column = [
        jnp.sum(jnp.where(same, place[axis : axis + 1, :], 0.0), axis=1, keepdims=True)
        for axis in range(2)
    ]
    for start in range(0, rows, SUM_ROWS):
        chunk = slice(start, start + SUM_ROWS)
        where_to = jnp.where(table[2:3, :] > 0.5, column[1][chunk, :], column[0][chunk, :])
        x_in_ref[chunk, :] = tokens[chunk, :].astype(jnp.float32) + sine(
            where_to * table[0:1, :], jnp.broadcast_to(table[1:2, :], where_to.shape)
        )
    angle = timestep[0].astype(jnp.float32) * jnp.broadcast_to(
        table[3:4, :freq_size], (SUM_ROWS, freq_size)
    )
    shifted = jnp.broadcast_to(table[4:5, :freq_size], (SUM_ROWS, freq_size))
    features = sine(angle, shifted).astype(jnp.bfloat16)
    for copy in copies[3:]:
        copy.wait()
    hidden = silu(jnp.dot(features, time_in[...], preferred_element_type=jnp.float32))
    cond = lax.dot_general(
        hidden.astype(jnp.bfloat16),
        time_out[...],
        (((1,), (1,)), ((), ())),
        preferred_element_type=jnp.float32,
    )
    partial = jnp.dot(
        silu(cond).astype(jnp.bfloat16), ada_weight[...], preferred_element_type=jnp.float32
    )
    x_in = x_in_ref[...]
    centered = x_in - jnp.mean(x_in, axis=1, keepdims=True)
    variance = jnp.mean(centered * centered, axis=1, keepdims=True)
    message[...] = (centered * lax.rsqrt(variance + 1e-06)).astype(jnp.bfloat16)
    sums[...] = pack_sums([partial[:, piece * width : (piece + 1) * width] for piece in range(3)])

    my_index = lax.axis_index("patch")
    key_id = lax.broadcasted_iota(jnp.int32, bias.shape, 1)
    valid = key_id < 0
    for block in range(parts):
        first = block * rows
        used = counts[part_index(my_index, block)]
        valid = jnp.logical_or(valid, jnp.logical_and(key_id >= first, key_id < first + used))
    bias[...] = jnp.where(valid, 0.0, neg_large)
    own_row = lax.broadcasted_iota(jnp.int32, row_valid.shape, 0)
    row_valid[...] = (own_row < counts[my_index]).astype(jnp.float32)


def pack_sums(pieces):
    row_id = lax.broadcasted_iota(jnp.int32, pieces[0].shape, 0)
    packed = jnp.zeros(pieces[0].shape, jnp.float32)
    for piece, value in enumerate(pieces):
        high, low = high_low(value)
        packed = jnp.where(row_id == 2 * piece, high.astype(jnp.float32), packed)
        packed = jnp.where(row_id == 2 * piece + 1, low.astype(jnp.float32), packed)
    return packed.astype(jnp.bfloat16)


def sum_piece(value, piece):
    return value[2 * piece : 2 * piece + 1, :] + value[2 * piece + 1 : 2 * piece + 2, :]


def add_kernel(*refs):
    out = refs[-1]
    total = sum(ref[...].astype(jnp.float32) for ref in refs[:-1])
    out[...] = pack_sums(
        [jnp.broadcast_to(sum_piece(total, piece), out.shape) for piece in range(3)]
    )


def attend_rows(query_ref, rows, key_bias, keys, values, out):
    width = keys.shape[1]
    head_size = width // HEADS
    base_two = math.log2(math.e) / math.sqrt(head_size)
    lse_lane = lax.broadcasted_iota(jnp.int32, (rows, LANES), 1)
    lse_all = jnp.zeros((rows, LANES), jnp.float32)
    windows = [(first, min(first + 2 * LANES, width)) for first in range(0, width, 2 * LANES)]
    inside = [
        [
            head
            for head in range(HEADS)
            if head * head_size < last and (head + 1) * head_size > first
        ]
        for first, last in windows
    ]
    scores, weights, inverse, tiles = {}, {}, {}, []

    def lanes_of(head, first, last):
        lane = lax.broadcasted_iota(jnp.int32, (1, last - first), 1) + first
        return jnp.logical_and(lane >= head * head_size, lane < (head + 1) * head_size)

    def score(index):
        first, last = windows[index]
        window = query_ref[:, first:last]
        stacked = jnp.concatenate(
            [
                jnp.where(lanes_of(head, first, last), window, jnp.zeros((), jnp.bfloat16))
                for head in inside[index]
            ],
            axis=0,
        )
        result = lax.dot_general(
            stacked,
            keys[:, first:last],
            (((1,), (1,)), ((), ())),
            preferred_element_type=jnp.float32,
        )
        for place, head in enumerate(inside[index]):
            part = result[place * rows : (place + 1) * rows, :]
            scores[head] = scores[head] + part if head in scores else part

    score(0)
    for index, (first, last) in enumerate(windows):
        if index + 1 < len(windows):
            score(index + 1)
        for head in inside[index]:
            if head in weights:
                continue
            value = scores.pop(head) + key_bias
            top = jnp.max(value, axis=1, keepdims=True)
            value = jnp.exp2((value - top) * base_two)
            total = jnp.sum(value, axis=1, keepdims=True)
            weights[head] = value.astype(jnp.bfloat16)
            inverse[head] = 1.0 / total
            lse_all = jnp.where(lse_lane == head, top * base_two + jnp.log2(total), lse_all)
        result = jnp.dot(
            jnp.concatenate([weights[head] for head in inside[index]], axis=0),
            values[:, first:last],
            preferred_element_type=jnp.float32,
        )
        joined = None
        for place, head in enumerate(inside[index]):
            part = result[place * rows : (place + 1) * rows, :] * inverse[head]
            if joined is None:
                joined = part
            else:
                joined = jnp.where(lanes_of(head, first, last), part, joined)
        tiles.append((first, last, joined.astype(jnp.bfloat16)))
    for first, last, tile in tiles:
        out[:, first:last] = tile
    out[:, width:] = pack_lse(lse_all)


def attend_kernel(block_rows, key_count, *refs):
    bias, sums_a, sums_b = refs[:3]
    key_refs = refs[3 : 3 + key_count]
    own, across, weight = refs[3 + key_count : 6 + key_count]
    own_query, keys, values, across_out = refs[6 + key_count : 10 + key_count]
    mod_keys, mod_queries, across_query = refs[10 + key_count :]
    width = weight.shape[0]
    sums = sums_a[...].astype(jnp.float32) + sums_b[...].astype(jnp.float32)
    shift = sum_piece(sums, 0)
    scale = 1.0 + sum_piece(sums, 1)

    def modulate(value):
        return (value.astype(jnp.float32) * scale + shift).astype(jnp.bfloat16)

    place = 0
    for ref in key_refs:
        for start in range(0, ref.shape[0], block_rows):
            mod_keys[place : place + block_rows, :] = modulate(ref[start : start + block_rows, :])
            place += block_rows
    mod_queries[:block_rows, :] = modulate(own[...])
    mod_queries[block_rows:, :] = modulate(across[...])
    for start in range(0, width, PIECE):
        stop = min(start + PIECE, width)
        both = jnp.dot(
            mod_queries[...], weight[:, start:stop], preferred_element_type=jnp.float32
        ).astype(jnp.bfloat16)
        own_query[:, start:stop] = both[:block_rows, :]
        across_query[:, start:stop] = both[block_rows:, :]
    for start in range(0, 2 * width, PIECE):
        stop = min(start + PIECE, 2 * width)
        both = jnp.dot(
            mod_keys[...], weight[:, width + start : width + stop], preferred_element_type=jnp.float32
        ).astype(jnp.bfloat16)
        split = min(max(width - start, 0), stop - start)
        if split:
            keys[:, start : start + split] = both[:, :split]
        if split < stop - start:
            values[:, start + split - width : stop - width] = both[:, split:]
    attend_rows(across_query, block_rows, bias[0:1, :], keys, values, across_out)


def own_kernel(bias, query, keys, values, out, lse, expand):
    width = query.shape[1]
    head_size = width // HEADS
    attend_rows(query, query.shape[0], bias[0:1, :], keys, values, out)
    lse[...] = unpack_lse(out[:, width:])
    head_id = lax.broadcasted_iota(jnp.int32, expand.shape, 0)
    lane_id = lax.broadcasted_iota(jnp.int32, expand.shape, 1)
    low = head_id * head_size
    inside = jnp.logical_and(lane_id >= low, lane_id < low + head_size)
    expand[...] = inside.astype(jnp.float32).astype(jnp.bfloat16)


def pack_lse(lse):
    high = lse.astype(jnp.bfloat16).astype(jnp.float32)
    middle = (lse - high).astype(jnp.bfloat16).astype(jnp.float32)
    low = lse - high - middle
    return (high + pltpu.roll(middle, HEADS, 1) + pltpu.roll(low, 2 * HEADS, 1)).astype(
        jnp.bfloat16
    )


def unpack_lse(packed):
    source = lax.broadcasted_iota(jnp.int32, (LANES, LANES), 0)
    target = lax.broadcasted_iota(jnp.int32, (LANES, LANES), 1)
    chosen = source == target
    for piece in range(1, 3):
        chosen = jnp.logical_or(chosen, source == target + piece * HEADS)
    chosen = jnp.logical_and(chosen, target < HEADS).astype(jnp.bfloat16)
    return jnp.dot(packed, chosen, preferred_element_type=jnp.float32)


def merge(value_a, lse_a, packed_b, expand):
    width = value_a.shape[1] - LANES
    lse_b = unpack_lse(packed_b[:, width:])
    top = jnp.maximum(lse_a, lse_b)
    part_a = jnp.exp2(lse_a - top)
    part_b = jnp.exp2(lse_b - top)
    high, rest = high_low(part_b / (part_a + part_b))
    share = jnp.dot(high, expand, preferred_element_type=jnp.float32) + jnp.dot(
        rest, expand, preferred_element_type=jnp.float32
    )
    first = value_a[:, :width].astype(jnp.float32)
    return first + share * (packed_b[:, :width].astype(jnp.float32) - first)


def finish_kernel(
    value_a, lse_a, expand, packed_b, x_in, row_valid, sums_a, sums_b, weight, out_far, out, sent
):
    width = out.shape[1]
    value = merge(value_a[...], lse_a[...], packed_b[...], expand[...]).astype(jnp.bfloat16)
    gate = sum_piece(sums_a[...].astype(jnp.float32) + sums_b[...].astype(jnp.float32), 2)
    copies = []
    for index, start in enumerate(range(0, width, FINISH_PIECE)):
        columns = slice(start, min(start + FINISH_PIECE, width))
        projected = jnp.dot(value, weight[:, columns], preferred_element_type=jnp.float32)
        out[:, columns] = (
            x_in[:, columns] + gate[:, columns] * projected * row_valid[:, 0:1]
        ).astype(jnp.bfloat16)
        size = columns.stop - columns.start
        copies.append(
            pltpu.make_async_copy(
                out.at[:, pl.ds(start, size)], out_far.at[:, pl.ds(start, size)], sent.at[index]
            )
        )
        copies[-1].start()
    for copy in copies:
        copy.wait()


def far():
    return pl.BlockSpec(memory_space=pltpu.HBM)


def stay_far(array):
    return pltpu.with_memory_space_constraint(array, pltpu.HBM)


def per_device(
    tokens, positions, counts, timestep, time_in, time_out, ada_weight, qkv_weight, out_weight
):
    devices = lax.axis_size("patch")
    rows, width = tokens.shape
    shape = jax.ShapeDtypeStruct
    table = jnp.asarray(lane_table(width, time_in.shape[0]))
    far_masks = [mask for mask in range(devices) if not mask & (CORE_MASK | MERGE_MASK)]
    key_masks = far_masks + [mask | CORE_MASK for mask in far_masks]
    direct = devices <= DIRECT_LIMIT

    def swap(value, mask):
        pairs = [(index, index ^ mask) for index in range(devices)]
        return lax.ppermute(value, "patch", pairs)

    def part_index(my_index, block):
        if direct:
            return jnp.bitwise_xor(my_index, key_masks[block])
        return jnp.bitwise_and(my_index, MERGE_MASK) + sorted(key_masks)[block]

    inputs = (timestep, counts, tokens, positions, table, time_in, time_out.T, ada_weight)
    message, sums, x_in, bias, row_valid = pl.pallas_call(
        functools.partial(front_kernel, part_index, len(key_masks)),
        out_shape=(
            shape((rows, width), jnp.bfloat16),
            shape((SUM_ROWS, width), jnp.bfloat16),
            shape((rows, width), jnp.float32),
            shape((SUM_ROWS, rows * len(key_masks)), jnp.float32),
            shape((rows, LANES), jnp.float32),
        ),
        in_specs=[pl.BlockSpec(memory_space=pltpu.SMEM)] + [far()] * (len(inputs) - 1),
        out_specs=(vmem(),) * 5,
        scratch_shapes=[
            (pltpu.SMEM if array.ndim == 1 else pltpu.VMEM)(array.shape, array.dtype)
            for array in inputs[1:]
        ]
        + [pltpu.SemaphoreType.DMA((len(inputs) - 1,))],
        compiler_params=grant(8),
        name="front",
    )(inputs[0], *[stay_far(array) for array in inputs[1:]])

    def add(*addends):
        return pl.pallas_call(
            add_kernel,
            out_shape=shape((SUM_ROWS, width), jnp.bfloat16),
            in_specs=[vmem()] * len(addends),
            out_specs=vmem(),
            compiler_params=grant(4),
            cost_estimate=pl.CostEstimate(
                flops=1 << 34, bytes_accessed=4 * qkv_weight.size, transcendentals=0
            ),
            name="add",
        )(*addends)

    across = swap(message, MERGE_MASK)
    if direct:
        near = [message] + [swap(message, mask) for mask in far_masks[1:]]
        key_parts = near + [swap(part, CORE_MASK) for part in near]
        running = add(sums, swap(sums, CORE_MASK))
        running = add(running, *[swap(running, mask) for mask in far_masks[1:]])
        half_sums = running
        other_sums = swap(running, MERGE_MASK)
    else:
        groups = [[mask | rest for mask in sorted(key_masks)] for rest in (0, MERGE_MASK)]
        key_parts = [lax.all_gather(message, "patch", axis_index_groups=groups, tiled=True)]
        running = sums
        step = 1
        while 2 * step < devices:
            running = add(running, swap(running, step))
            step *= 2
        half_sums = running
        other_sums = swap(running, step)

    total_keys = rows * len(key_masks)
    own_query, keys, values, send = pl.pallas_call(
        functools.partial(attend_kernel, rows, len(key_parts)),
        out_shape=(
            shape((rows, width), jnp.bfloat16),
            shape((total_keys, width), jnp.bfloat16),
            shape((total_keys, width), jnp.bfloat16),
            shape((rows, width + LANES), jnp.bfloat16),
        ),
        in_specs=[vmem()] * (6 + len(key_parts)),
        out_specs=(vmem(),) * 4,
        scratch_shapes=[
            pltpu.VMEM((total_keys, width), jnp.bfloat16),
            pltpu.VMEM((2 * rows, width), jnp.bfloat16),
            pltpu.VMEM((rows, width), jnp.bfloat16),
        ],
        compiler_params=grant(ATTEND_GRANT if direct else 56),
        name="attend",
    )(bias, half_sums, other_sums, *key_parts, message, across, qkv_weight)
    own, own_lse, expand = pl.pallas_call(
        own_kernel,
        out_shape=(
            shape((rows, width + LANES), jnp.bfloat16),
            shape((rows, LANES), jnp.float32),
            shape((LANES, width), jnp.bfloat16),
        ),
        in_specs=[vmem()] * 4,
        out_specs=(vmem(),) * 3,
        compiler_params=grant(8 if direct else 40),
        cost_estimate=pl.CostEstimate(
            flops=1 << 34, bytes_accessed=4 * keys.size, transcendentals=0
        ),
        name="own",
    )(bias, own_query, keys, values)
    return pl.pallas_call(
        finish_kernel,
        out_shape=shape((rows, width), jnp.bfloat16),
        in_specs=[vmem()] * 9,
        out_specs=far(),
        scratch_shapes=[
            pltpu.VMEM((rows, width), jnp.bfloat16),
            pltpu.SemaphoreType.DMA((-(-width // FINISH_PIECE),)),
        ],
        compiler_params=grant(8),
        name="finish",
    )(
        own,
        own_lse,
        expand,
        swap(send, MERGE_MASK),
        x_in,
        row_valid,
        half_sums,
        other_sums,
        out_weight,
    )


def solution(mesh):
    placed = (
        P(("req", "patch"), None),
        P(None, ("req", "patch")),
        P("req"),
        P("req"),
        P(),
        P(None, "patch"),
        P("patch", None),
        P(),
        P(),
    )

    return jax.shard_map(
        per_device, mesh=mesh, in_specs=placed, out_specs=P(("req", "patch"), None), check_vma=False
    )
```
